512 devices in a mesh: seq: 32 (over z, core), ch: 16 (over x, y).
Axes of the slice: x: 4, y: 4, z: 16, core: 2. Of those that a mesh axis runs over, the one named last changes fastest.
Arguments:
- input_q: bfloat16 [16384, 8192], P('seq', 'ch'), may hold values from -6 to 6
- input_k: bfloat16 [16384, 8192], P('seq', 'ch'), may hold values from -6 to 6
- input_v: bfloat16 [16384, 8192], P('seq', 'ch'), may hold values from -6 to 6
- grad_out: bfloat16 [16384, 8192], P('seq', 'ch'), may hold values from -6 to 6
- short_filters: float32 [3, 3, 8192], P(None, None, 'ch'), may hold values from -3.5 to 3.5
- long_filter: float32 [128, 8192], P(None, 'ch'), may hold values from -0.5 to 0.5
- skip_gain: float32 [8192], P('ch'), may hold values from 0.5 to 1.5
Outputs:
- grad_input_q: bfloat16 [16384, 8192], P('seq', 'ch')
- grad_input_k: bfloat16 [16384, 8192], P('seq', 'ch')
- grad_input_v: bfloat16 [16384, 8192], P('seq', 'ch')
- grad_long: float32 [128, 8192], P('seq', 'ch')
- grad_short: float32 [3, 3, 8192], P(None, None, 'ch')
- grad_skip: float32 [8192], P('ch')
The draws below stay inside these ranges and needn't reach their ends.
All inputs are finite; a program needn't handle non-finite values.
Results may differ from the reference program's by a relative error of at most 0.001.
Values may be sent and summed in bfloat16 or wider, within the bound.
A program may use at most 64 MiB of HBM per device.

```python
import math
import jax
import jax.numpy as jnp
from jax import lax

D = 8192
TAPS = 3
FILT = 128
SEQ = 16384


def levels(stream_key, shape, shards, smallest, high):
    level, own = 1.0, jax.random.fold_in(stream_key, 6)
    for axis_at, shards_of in shards:
        draws = jnp.exp(jax.random.uniform(jax.random.fold_in(own, axis_at), (shards_of,), jnp.float32, smallest / len(shards), high / len(shards)))
        level = level * jnp.repeat(draws, shape[axis_at] // shards_of).reshape([-1 if axis == axis_at else 1 for axis in range(len(shape))])
    return level


def gaussian(key, dims, scale, limit, cuts=(), dtype=jnp.bfloat16):
    factor_of = levels(key, dims, cuts, -0.22, 0.18) if cuts else 1.0
    entries = jax.random.normal(key, dims, jnp.float32) * scale * factor_of
    return jnp.minimum(jnp.maximum(entries, -limit), limit).astype(dtype)


def setup_inputs(seed: int = 0) -> dict:
    arg_keys = jax.random.split(jax.random.key(seed), 8)
    return {
        "input_q": gaussian(arg_keys[0], (SEQ, D), 1.0, 6.0, ((0, 32), (1, 16))),
        "input_k": gaussian(arg_keys[1], (SEQ, D), 1.0, 6.0, ((0, 32), (1, 16))),
        "input_v": gaussian(arg_keys[2], (SEQ, D), 1.0, 6.0, ((0, 32), (1, 16))),
        "grad_out": gaussian(arg_keys[3], (SEQ, D), 1.0, 6.0, ((0, 32), (1, 16))),
        "short_filters": gaussian(arg_keys[4], (3, TAPS, D), TAPS ** -0.5, 3.5, ((2, 16),), jnp.float32),
        "long_filter": gaussian(arg_keys[5], (FILT, D), FILT ** -0.5, 0.5, ((1, 16),), jnp.float32),
        "skip_gain": jnp.clip(0.5 + 1.0 * jax.random.uniform(arg_keys[6], (D,), jnp.float32) ** levels(arg_keys[6], (D,), ((0, 16),), -0.2, 0.2), 0.5, 1.5),
    }


def one_block(packed):
    query_in, key_in, value_in, upstream, taps_w, filt, gain = packed
    length = query_in.shape[0]
    ntap = taps_w.shape[1]

    def short_conv(signal, weights):
        padded = jnp.pad(signal, ((ntap - 1, 0), (0, 0)))
        total = jnp.zeros_like(signal)
        for index in range(ntap):
            total = total + weights[index] * padded[ntap - 1 - index:ntap - 1 - index + length]
        return total

    def short_back(grad, weights, signal):
        grad_pad = jnp.pad(grad, ((0, ntap - 1), (0, 0)))
        sig_pad = jnp.pad(signal, ((ntap - 1, 0), (0, 0)))
        result = jnp.zeros_like(grad)
        rows_taps = []
        for index in range(ntap):
            result = result + weights[index] * grad_pad[index:index + length]
            rows_taps.append(jnp.sum(grad * sig_pad[ntap - 1 - index:ntap - 1 - index + length], axis=0))
        return result, jnp.stack(rows_taps)

    q_sig = query_in.astype(jnp.float32)
    k_sig = key_in.astype(jnp.float32)
    v_sig = value_in.astype(jnp.float32)
    dy_sig = upstream.astype(jnp.float32)
    q_feat = short_conv(q_sig, taps_w[0])
    k_feat = short_conv(k_sig, taps_w[1])
    v_feat = short_conv(v_sig, taps_w[2])
    z_feat = k_feat * v_feat
    double = 2 * length
    spec_h = jnp.fft.rfft(filt, n=double, axis=0)
    spec_z = jnp.fft.rfft(z_feat, n=double, axis=0)
    s_feat = jnp.fft.irfft(spec_z * spec_h, n=double, axis=0)[:length].astype(jnp.float32) + gain * z_feat
    grad_q = dy_sig * s_feat
    grad_s = dy_sig * q_feat
    spec_s = jnp.fft.rfft(grad_s, n=double, axis=0)
    grad_z = jnp.fft.irfft(spec_s * jnp.conj(spec_h), n=double, axis=0)[:length].astype(jnp.float32) + gain * grad_s
    grad_k = grad_z * v_feat
    grad_v = grad_z * k_feat
    grad_filt = jnp.fft.irfft(spec_s * jnp.conj(spec_z), n=double, axis=0)[:filt.shape[0]].astype(jnp.float32)
    grad_gain = jnp.sum(grad_s * z_feat, axis=0)
    back_q, taps_q = short_back(grad_q, taps_w[0], q_sig)
    back_k, taps_k = short_back(grad_k, taps_w[1], k_sig)
    back_v, taps_v = short_back(grad_v, taps_w[2], v_sig)
    return (back_q.astype(jnp.bfloat16), back_k.astype(jnp.bfloat16), back_v.astype(jnp.bfloat16),
            grad_filt, jnp.stack([taps_q, taps_k, taps_v]), grad_gain)


def reference(input_q, input_k, input_v, grad_out, short_filters, long_filter, skip_gain):
    length, width = input_q.shape
    block = math.gcd(width, 512)
    count = width // block

    def split(array):
        return array.reshape(array.shape[0], count, block).transpose(1, 0, 2)

    def merge(array):
        return array.transpose(1, 0, 2).reshape(array.shape[1], width)

    packed = (split(input_q), split(input_k), split(input_v), split(grad_out),
              short_filters.reshape(3, short_filters.shape[1], count, block).transpose(2, 0, 1, 3),
              split(long_filter), skip_gain.reshape(count, block))
    back_q, back_k, back_v, grad_filt, grad_taps, grad_gain = lax.map(one_block, packed)
    grad_taps = grad_taps.transpose(1, 2, 0, 3).reshape(3, short_filters.shape[1], width)
    return (merge(back_q), merge(back_k), merge(back_v), merge(grad_filt), grad_taps, grad_gain.reshape(width))
```

```python
import functools

import jax
import jax.numpy as jnp
import ml_dtypes
import numpy as np
from jax import lax
from jax.experimental import pallas as pl
from jax.experimental.pallas import tpu as pltpu
from jax.sharding import PartitionSpec as P

F32, BF16 = jnp.float32, jnp.bfloat16
BLK = 128
ROWS = 16


def tables():
    order = np.concatenate([np.arange(0, BLK, 2), np.arange(1, BLK, 2)])
    angle = np.outer(np.pi * (2 * order + 1) / (2 * BLK), np.arange(BLK))
    full = np.concatenate([np.cos(angle), -np.sin(angle)], 0)
    high = full.astype(ml_dtypes.bfloat16).astype(np.float64)
    low = full - high
    fwd = np.concatenate([high, high, low], 1)
    inv = np.concatenate([high.T, high.T, low.T], 1) / BLK
    return fwd.astype(ml_dtypes.bfloat16), inv.astype(ml_dtypes.bfloat16)


def kernel(
    chips,
    q_hbm, k_hbm, v_hbm, y_hbm, sf_hbm, lf_hbm, sg_hbm, fwd_hbm, inv_hbm,
    oq, ok, ov, ofilt, otaps, ogain,
    qb, kb, vb, yb, nq, ny, sf, lf, sg, fwd, inv,
    kf, vf, s_t, gz_t, xz, xg, xh, zs, gs, hs, xs, xu, gl_f, xgl,
    mine3, nx, glt, gl_in, racc, rs_in, small, half, half_in, ar, fin,
    in_sem, send, recv, known,
):
    length = q_hbm.shape[0]
    width = q_hbm.shape[1]
    nblk = length // BLK
    me = lax.axis_index("seq")
    total = 2 * chips
    z, c = me // 2, lax.rem(me, 2)
    has_prev, has_next = me > 0, me < total - 1
    prev, nxt = me - 1, me + 1
    partner = me + 1 - 2 * c

    def at_chip(chip):
        return lax.rem(chip + chips, chips) * 2 + c

    def remote(src, dst, slot, device):
        return pltpu.make_async_remote_copy(
            src_ref=src, dst_ref=dst, send_sem=send.at[slot], recv_sem=recv.at[slot],
            device_id={"seq": device}, device_id_type=pl.DeviceIdType.MESH,
        )

    def signal(sem, device):
        pl.semaphore_signal(sem, 1, device_id={"seq": device}, device_id_type=pl.DeviceIdType.MESH)

    def load(array, b):
        hbm, buf = ((q_hbm, qb), (k_hbm, kb), (v_hbm, vb), (y_hbm, yb))[array]
        off = 0 if array == 3 else ROWS
        return pltpu.make_async_copy(
            hbm.at[pl.ds(b * BLK, BLK)], buf.at[pl.ds(off + b * BLK, BLK)], in_sem.at[array * nblk + b]
        )

    extra = []
    for n, (hbm, buf) in enumerate(((sf_hbm, sf), (lf_hbm, lf), (sg_hbm, sg), (fwd_hbm, fwd), (inv_hbm, inv))):
        extra.append(pltpu.make_async_copy(hbm, buf, in_sem.at[4 * nblk + n]))

    last = nblk - 1
    barrier = pltpu.get_barrier_semaphore()
    extra[0].start()
    for b in (last - 1, last):
        load(1, b).start()
        load(2, b).start()
    signal(barrier, at_chip(z + 1))
    signal(barrier, at_chip(z - 1))

    @pl.when(has_prev)
    def _():
        signal(barrier, prev)

    @pl.when(has_next)
    def _():
        signal(barrier, nxt)

    load(0, 0).start()
    load(3, 0).start()
    extra[1].start()
    extra[2].start()
    extra[3].start()
    load(0, last).start()
    for b in range(nblk):
        for array in range(4):
            if not (array in (1, 2) and b >= last - 1) and not (array in (0, 3) and b == 0) and not (array == 0 and b == last):
                load(array, b).start()
    extra[4].start()

    @pl.when(jnp.logical_not(has_prev))
    def _():
        for buf in (qb, kb, vb):
            buf[0:ROWS, :] = jnp.zeros((ROWS, width), BF16)
        xz[0, 0 : 2 * BLK, :] = jnp.zeros((2 * BLK, width), BF16)

    @pl.when(jnp.logical_not(has_next))
    def _():
        nq[...] = jnp.zeros_like(nq)
        ny[...] = jnp.zeros_like(ny)
        xg[nblk, 0 : 2 * BLK, :] = jnp.zeros((2 * BLK, width), BF16)
        nx[...] = jnp.zeros_like(nx)

    def delayed(now, before):
        cat = jnp.concatenate([before.astype(F32)[8:], now.astype(F32)], 0)
        return cat[8:], pltpu.roll(cat, 1, 0)[8:], pltpu.roll(cat, 2, 0)[8:]

    def feat(now, before, which):
        own, one, two = delayed(now, before)
        return sf[which, 0:1, :] * own + sf[which, 1:2, :] * one + sf[which, 2:3, :] * two

    def put(ref, b, n, value):
        high = value.astype(BF16)
        low = (value - high.astype(F32)).astype(BF16)
        ref[b, pl.ds(n, ROWS), :] = high
        ref[b, pl.ds(BLK + n, ROWS), :] = low
        ref[b, pl.ds(2 * BLK + n, ROWS), :] = high

    def z_chunk(b, n):
        row = b * BLK + n
        kk = feat(kb[pl.ds(row + ROWS, ROWS), :], kb[pl.ds(row, ROWS), :], 1)
        vv = feat(vb[pl.ds(row + ROWS, ROWS), :], vb[pl.ds(row, ROWS), :], 2)
        kf[pl.ds(row, ROWS), :] = kk
        vf[pl.ds(row, ROWS), :] = vv
        put(xz, b + 1, n, kk * vv)

    def g_chunk(b, n):
        row = b * BLK + n
        qq = feat(qb[pl.ds(row + ROWS, ROWS), :], qb[pl.ds(row, ROWS), :], 0)
        put(xg, b, n, yb[pl.ds(row, ROWS), :].astype(F32) * qq)

    def chunks(body, first, stop):
        def step(i, carry):
            body(pl.multiple_of(i * ROWS, ROWS))
            return carry

        lax.fori_loop(first, stop, step, 0)

    per = BLK // ROWS
    extra[0].wait()
    for b in (last - 1, last):
        load(1, b).wait()
        load(2, b).wait()
    chunks(lambda n: z_chunk(last, n), 0, per)
    load(0, 0).wait()
    load(3, 0).wait()
    chunks(lambda n: g_chunk(0, n), 1, per)
    load(0, last).wait()

    count = 2 + has_prev.astype(jnp.int32) + has_next.astype(jnp.int32)
    pl.semaphore_wait(barrier, count)
    tail = pl.ds(length, ROWS)
    to_next = [remote(buf.at[tail], buf.at[pl.ds(0, ROWS)], n, nxt) for n, buf in enumerate((qb, kb, vb))]
    z_halo = remote(xz.at[nblk, pl.ds(0, 2 * BLK)], xz.at[0, pl.ds(0, 2 * BLK)], 3, nxt)
    to_prev = [
        remote(qb.at[pl.ds(ROWS, ROWS)], nq, 4, prev),
        remote(yb.at[pl.ds(0, ROWS)], ny, 5, prev),
    ]
    g_halo = [
        remote(xg.at[0, pl.ds(h * BLK + ROWS, BLK - ROWS)], xg.at[nblk, pl.ds(h * BLK + ROWS, BLK - ROWS)], 6 + h, prev)
        for h in range(2)
    ]

    @pl.when(has_next)
    def _():
        for copy in to_next:
            copy.start()
        z_halo.start()

    @pl.when(has_prev)
    def _():
        for copy in to_prev + g_halo:
            copy.start()

    steps = []
    radius = 1
    while radius < chips // 2:
        steps.append(radius)
        radius *= 2

    def tell(n):
        if n < len(steps):
            signal(known.at[n], at_chip(z + steps[n]))
            signal(known.at[n], at_chip(z - steps[n]))

    def learn(n):
        if n < len(steps):
            pl.semaphore_wait(known.at[n], 2)

    tell(0)

    extra[1].wait()
    extra[2].wait()

    def h_chunk(n):
        put(xh, 0, n, lf[pl.ds(n, ROWS), :])

    chunks(h_chunk, 1, per)
    first = lf[0:ROWS, :]
    at_zero = lax.broadcasted_iota(jnp.int32, (ROWS, width), 0) == 0
    put(xh, 0, 0, jnp.where(at_zero, first + sg[...], first))
    extra[3].wait()

    def dft(x, b, out, o):
        for lane in range(0, width, 256):
            cols = slice(lane, lane + 256)
            out[o, :, cols] = jnp.dot(fwd[...], x[b, :, cols], preferred_element_type=F32)

    def inverse(x, b):
        return jnp.dot(inv[...], x[b], preferred_element_type=F32)

    dft(xh, 0, hs, 0)
    for b in range(last):
        load(1, b).wait() if b < last - 1 else None
        load(2, b).wait() if b < last - 1 else None
        chunks(functools.partial(z_chunk, b), 1 if b == 0 else 0, per)
    for b in range(1, nblk):
        load(0, b).wait() if b < last else None
        load(3, b).wait()
        chunks(functools.partial(g_chunk, b), 0, per)
    learn(0)
    tell(1)
    for b in range(1, nblk):
        dft(xz, b + 1, zs, b + 1)
        dft(xg, b, gs, b)
    learn(1)
    tell(2)

    @pl.when(has_prev)
    def _():
        for copy in to_next:
            copy.wait_recv()

    z_chunk(0, 0)
    g_chunk(0, 0)
    dft(xz, 1, zs, 1)
    dft(xg, 0, gs, 0)
    extra[4].wait()

    def put_spectrum(ref, b, k, lanes, real, imag):
        for off, value in ((0, real), (BLK, imag)):
            high = value.astype(BF16)
            low = (value - high.astype(F32)).astype(BF16)
            ref[b, pl.ds(off + k, ROWS), lanes] = high
            ref[b, pl.ds(2 * BLK + off + k, ROWS), lanes] = low
            ref[b, pl.ds(4 * BLK + off + k, ROWS), lanes] = high

    def by_frequency(body):
        for sign, start in ((1.0, 0), (-1.0, BLK // 2)):
            for lane in range(0, width, 256):

                def step(i, carry, sign=sign, start=start, lane=lane):
                    body(pl.multiple_of(start + i * ROWS, ROWS), slice(lane, lane + 256), sign)
                    return carry

                lax.fori_loop(0, BLK // 2 // ROWS, step, 0)

    def add(a, sign, b):
        return a + b if sign > 0 else a - b

    def z_spectrum(b, start, k, lanes, sign):
        re, im = pl.ds(k, ROWS), pl.ds(BLK + k, ROWS)
        vr = add(zs[b + 1, re, lanes], -sign, zs[b, im, lanes])
        vi = add(zs[b + 1, im, lanes], sign, zs[b, re, lanes])
        hr, hi = hs[0, re, lanes], hs[0, im, lanes]
        put_spectrum(xs, b, k, lanes, hr * vr - hi * vi, hr * vi + hi * vr)
        gr, gi = gs[b, re, lanes], gs[b, im, lanes]
        lr, li = gr * vr + gi * vi, gi * vr - gr * vi
        if not start:
            lr, li = gl_f[re, lanes] + lr, gl_f[im, lanes] + li
        return lr, li

    def z_stage(b, start, final):
        def body(k, lanes, sign):
            lr, li = z_spectrum(b, start, k, lanes, sign)
            if final:
                put_spectrum(xgl, 0, k, lanes, lr, li)
            else:
                gl_f[pl.ds(k, ROWS), lanes] = lr
                gl_f[pl.ds(BLK + k, ROWS), lanes] = li

        by_frequency(body)

    def g_stage(b):
        def body(k, lanes, sign):
            re, im = pl.ds(k, ROWS), pl.ds(BLK + k, ROWS)
            ur = add(gs[b, re, lanes], sign, gs[b + 1, im, lanes])
            ui = add(gs[b, im, lanes], -sign, gs[b + 1, re, lanes])
            hr, hi = hs[0, re, lanes], hs[0, im, lanes]
            put_spectrum(xu, b, k, lanes, hr * ur + hi * ui, hr * ui - hi * ur)

        by_frequency(body)

    def out_rows(b):
        return slice(b * BLK, (b + 1) * BLK)

    for b in range(1, nblk):
        z_stage(b, b == 1, False)
        s_t[out_rows(b), :] = inverse(xs, b)
    for b in range(last):
        g_stage(b)
        gz_t[out_rows(b), :] = inverse(xu, b)

    @pl.when(has_prev)
    def _():
        z_halo.wait_recv()

    xz[0, 2 * BLK :, :] = xz[0, 0:BLK, :]
    dft(xz, 0, zs, 0)
    z_stage(0, False, True)
    gl = inverse(xgl, 0)
    share = BLK // total
    for i in range(total):
        glt[i % 2, i // 2] = gl[share * i : share * (i + 1), :]
    small[9:10, :] = gl[0:1, :]
    to_partner = remote(glt.at[1 - c], gl_in, 8, partner)
    to_partner.start()

    s_t[out_rows(0), :] = inverse(xs, 0)
    row = lax.broadcasted_iota(jnp.int32, (8, width), 0)
    gq8 = yb[0:ROWS, :].astype(F32)[0:8] * s_t[0:8, :]
    gk8 = gz_t[0:8, :] * vf[0:8, :]
    gv8 = gz_t[0:8, :] * kf[0:8, :]
    mine3[...] = jnp.where(row < 2, gq8, jnp.where(row < 4, pltpu.roll(gk8, 2, 0), pltpu.roll(gv8, 4, 0)))
    firsts = remote(mine3, nx, 9, prev)

    @pl.when(has_prev)
    def _():
        firsts.start()

    learn(2)
    to_partner.wait_recv()
    racc[...] = glt[c] + gl_in[...]
    scatter = []
    order = sorted(range(1, chips), key=lambda d: (-min(d, chips - d), d))
    for d in order:
        chip = lax.rem(z + d, chips)
        copy = remote(racc.at[chip], rs_in.at[d], 16 + d, at_chip(chip))
        copy.start()
        scatter.append(copy)

    @pl.when(has_next)
    def _():
        for copy in to_prev + g_halo:
            copy.wait_recv()

    put(xg, nblk, 0, ny[...].astype(F32) * feat(nq[...], qb[tail, :], 0))
    xg[nblk, 2 * BLK + ROWS :, :] = xg[nblk, ROWS:BLK, :]
    dft(xg, nblk, gs, nblk)
    g_stage(last)
    gz_t[out_rows(last), :] = inverse(xu, last)

    def q_rows(row, n):
        return yb[pl.ds(row, ROWS), :].astype(F32)[0:n] * s_t[pl.ds(row, n), :]

    def k_rows(row, n):
        return gz_t[pl.ds(row, n), :] * vf[pl.ds(row, n), :]

    def v_rows(row, n):
        return gz_t[pl.ds(row, n), :] * kf[pl.ds(row, n), :]

    def back(which, rows_of, raw, out, row, after, sums):
        grad = rows_of(row, ROWS)
        cat = jnp.concatenate([grad, rows_of(row + ROWS, 8) if after is None else after], 0)
        one = pltpu.roll(cat, ROWS + 7, 0)[0:ROWS]
        two = pltpu.roll(cat, ROWS + 6, 0)[0:ROWS]
        value = sf[which, 0:1, :] * grad + sf[which, 1:2, :] * one + sf[which, 2:3, :] * two
        out[pl.ds(row, ROWS), :] = value.astype(BF16)
        parts = delayed(raw[pl.ds(row + ROWS, ROWS), :], raw[pl.ds(row, ROWS), :])
        products = [grad * part for part in parts]
        return tuple(s + p[0:8] + p[8:16] for s, p in zip(sums, products))

    kinds = ((0, q_rows, qb, oq), (1, k_rows, kb, ok), (2, v_rows, vb, ov))
    sums = []
    for which, rows_of, raw, out in kinds:

        def step(i, carry, which=which, rows_of=rows_of, raw=raw, out=out):
            return back(which, rows_of, raw, out, pl.multiple_of(i * ROWS, ROWS), None, carry)

        zero = jnp.zeros((8, width), F32)
        sums.append(lax.fori_loop(0, length // ROWS - 1, step, (zero, zero, zero)))

    @pl.when(has_next)
    def _():
        firsts.wait_recv()

    after = nx[...]
    afters = (after, pltpu.roll(after, 6, 0), pltpu.roll(after, 4, 0))
    for (which, rows_of, raw, out), carry, rows in zip(kinds, sums, afters):
        carry = back(which, rows_of, raw, out, length - ROWS, rows, carry)
        for i in range(3):
            small[3 * which + i : 3 * which + i + 1, :] = jnp.sum(carry[i], axis=0, keepdims=True)

    row = lax.broadcasted_iota(jnp.int32, (8, 128), 0)
    for h in range(2):
        lane = 256 * h
        half[h, 0] = small[0:8, lane : lane + 128]
        half[h, 1] = small[0:8, lane + 128 : lane + 256]
        half[h, 2] = jnp.where(
            row < 2,
            small[8:16, lane : lane + 128],
            jnp.where(row < 4, pltpu.roll(small[8:16, lane + 128 : lane + 256], 2, 0), 0.0),
        )
    halves = remote(half.at[1 - c], half_in, 10, partner)
    halves.start()
    halves.wait_recv()
    ar[z] = half[c] + half_in[...]
    spread = []
    for d in order:
        copy = remote(ar.at[z], ar.at[z], 16 + chips + d, at_chip(z + d))
        copy.start()
        spread.append(copy)

    for copy in scatter:
        copy.wait_recv()
    taps = racc[z]
    for d in range(1, chips):
        taps = taps + rs_in[d]
    ofilt[...] = taps

    for copy in spread:
        copy.wait_recv()
    whole = ar[0]
    for chip in range(1, chips):
        whole = whole + ar[chip]
    fin[c] = whole
    final = remote(fin.at[c], fin.at[c], 11, partner)
    final.start()
    final.wait_recv()
    for h in range(2):
        for j in range(2):
            cols = slice(256 * h + 128 * j, 256 * h + 128 * (j + 1))
            for i in range(8):
                otaps[i // 3, i % 3 : i % 3 + 1, cols] = fin[h, j, i : i + 1, :]
            otaps[2, 2:3, cols] = fin[h, 2, 2 * j : 2 * j + 1, :]
            ogain[0:1, cols] = fin[h, 2, 2 * j + 1 : 2 * j + 2, :]

    @pl.when(has_next)
    def _():
        for copy in to_next:
            copy.wait_send()
        z_halo.wait_send()

    @pl.when(has_prev)
    def _():
        for copy in to_prev + g_halo + [firsts]:
            copy.wait_send()

    for copy in [to_partner, halves, final] + scatter + spread:
        copy.wait_send()


def body(fwd, inv, chips, input_q, input_k, input_v, grad_out, short_filters, long_filter, skip_gain):
    length, width = input_q.shape
    nblk = length // BLK
    reach = length + ROWS
    hbm = pl.BlockSpec(memory_space=pl.ANY)
    vmem = pl.BlockSpec(memory_space=pltpu.VMEM)
    scratch = [
        *(pltpu.VMEM((reach, width), BF16) for _ in range(3)),
        pltpu.VMEM((length, width), BF16),
        pltpu.VMEM((ROWS, width), BF16),
        pltpu.VMEM((ROWS, width), BF16),
        pltpu.VMEM(short_filters.shape, F32),
        pltpu.VMEM(long_filter.shape, F32),
        pltpu.VMEM((1, width), F32),
        pltpu.VMEM(fwd.shape, BF16),
        pltpu.VMEM(inv.shape, BF16),
        *(pltpu.VMEM((length, width), F32) for _ in range(4)),
        pltpu.VMEM((nblk + 1, 3 * BLK, width), BF16),
        pltpu.VMEM((nblk + 1, 3 * BLK, width), BF16),
        pltpu.VMEM((1, 3 * BLK, width), BF16),
        pltpu.VMEM((nblk + 1, 2 * BLK, width), F32),
        pltpu.VMEM((nblk + 1, 2 * BLK, width), F32),
        pltpu.VMEM((1, 2 * BLK, width), F32),
        pltpu.VMEM((nblk, 6 * BLK, width), BF16),
        pltpu.VMEM((nblk, 6 * BLK, width), BF16),
        pltpu.VMEM((2 * BLK, width), F32),
        pltpu.VMEM((1, 6 * BLK, width), BF16),
        pltpu.VMEM((8, width), F32),
        pltpu.VMEM((8, width), F32),
        pltpu.VMEM((2, chips, BLK // (2 * chips), width), F32),
        pltpu.VMEM((chips, BLK // (2 * chips), width), F32),
        pltpu.VMEM((chips, BLK // (2 * chips), width), F32),
        pltpu.VMEM((chips, BLK // (2 * chips), width), F32),
        pltpu.VMEM((16, width), F32),
        pltpu.VMEM((2, 3, 8, 128), F32),
        pltpu.VMEM((3, 8, 128), F32),
        pltpu.VMEM((chips, 3, 8, 128), F32),
        pltpu.VMEM((2, 3, 8, 128), F32),
        pltpu.SemaphoreType.DMA((4 * nblk + 5,)),
        pltpu.SemaphoreType.DMA((16 + 2 * chips,)),
        pltpu.SemaphoreType.DMA((16 + 2 * chips,)),
        pltpu.SemaphoreType.REGULAR((3,)),
    ]
    outs = pl.pallas_call(
        functools.partial(kernel, chips),
        out_shape=(
            *(jax.ShapeDtypeStruct((length, width), BF16) for _ in range(3)),
            jax.ShapeDtypeStruct((BLK // (2 * chips), width), F32),
            jax.ShapeDtypeStruct(short_filters.shape, F32),
            jax.ShapeDtypeStruct((1, width), F32),
        ),
        in_specs=[hbm] * 9,
        out_specs=(vmem,) * 6,
        scratch_shapes=scratch,
        compiler_params=pltpu.CompilerParams(
            collective_id=0, has_side_effects=True, vmem_limit_bytes=48 * 1024 * 1024
        ),
        name="hyena_backward",
    )(input_q, input_k, input_v, grad_out, short_filters, long_filter, skip_gain[None], fwd, inv)
    return (*outs[:5], outs[5][0])


def solution(mesh):
    chips = mesh.shape["seq"] // 2
    fwd, inv = tables()

    def run(*arrays):
        return body(jnp.asarray(fwd), jnp.asarray(inv), chips, *arrays)

    return jax.shard_map(
        run,
        mesh=mesh,
        in_specs=(
            P("seq", "ch"),
            P("seq", "ch"),
            P("seq", "ch"),
            P("seq", "ch"),
            P(None, None, "ch"),
            P(None, "ch"),
            P("ch"),
        ),
        out_specs=(
            P("seq", "ch"),
            P("seq", "ch"),
            P("seq", "ch"),
            P("seq", "ch"),
            P(None, None, "ch"),
            P("ch"),
        ),
        check_vma=False,
    )
```

```python
import functools

import jax
import jax.numpy as jnp
import ml_dtypes
import numpy as np
from jax import lax
from jax.experimental import pallas as pl
from jax.experimental.pallas import tpu as pltpu
from jax.sharding import PartitionSpec as P

F32, BF16 = jnp.float32, jnp.bfloat16
BLK = 128
ROWS = 16


def tables():
    order = np.concatenate([np.arange(0, BLK, 2), np.arange(1, BLK, 2)])
    angle = np.outer(np.pi * (2 * order + 1) / (2 * BLK), np.arange(BLK))
    full = np.concatenate([np.cos(angle), -np.sin(angle)], 0)
    high = full.astype(ml_dtypes.bfloat16).astype(np.float64)
    low = full - high
    fwd = np.concatenate([high, high, low], 1)
    inv = np.concatenate([high.T, high.T, low.T], 1) / BLK
    return fwd.astype(ml_dtypes.bfloat16), inv.astype(ml_dtypes.bfloat16)


def kernel(
    chips,
    q_hbm, k_hbm, v_hbm, y_hbm, sf_hbm, lf_hbm, sg_hbm, fwd_hbm, inv_hbm,
    oq, ok, ov, ofilt, otaps, ogain,
    qb, kb, vb, yb, nq, ny, sf, lf, sg, fwd, inv,
    kf, vf, s_t, gz_t, xz, xg, xh, zs, gs, hs, xs, xu, gl_f, xgl,
    mine3, nx, glt, gl_in, racc, rs_in, small, half, half_in, ar, fin,
    in_sem, send, recv, known,
):
    length = q_hbm.shape[0]
    width = q_hbm.shape[1]
    nblk = length // BLK
    me = lax.axis_index("seq")
    total = 2 * chips
    z, c = me // 2, lax.rem(me, 2)
    has_prev, has_next = me > 0, me < total - 1
    prev, nxt = me - 1, me + 1
    partner = me + 1 - 2 * c

    def at_chip(chip):
        return lax.rem(chip + chips, chips) * 2 + c

    def remote(src, dst, slot, device):
        return pltpu.make_async_remote_copy(
            src_ref=src, dst_ref=dst, send_sem=send.at[slot], recv_sem=recv.at[slot],
            device_id={"seq": device}, device_id_type=pl.DeviceIdType.MESH,
        )

    def signal(sem, device):
        pl.semaphore_signal(sem, 1, device_id={"seq": device}, device_id_type=pl.DeviceIdType.MESH)

    def load(array, b):
        hbm, buf = ((q_hbm, qb), (k_hbm, kb), (v_hbm, vb), (y_hbm, yb))[array]
        off = 0 if array == 3 else ROWS
        return pltpu.make_async_copy(
            hbm.at[pl.ds(b * BLK, BLK)], buf.at[pl.ds(off + b * BLK, BLK)], in_sem.at[array * nblk + b]
        )

    extra = []
    for n, (hbm, buf) in enumerate(((sf_hbm, sf), (lf_hbm, lf), (sg_hbm, sg), (fwd_hbm, fwd), (inv_hbm, inv))):
        extra.append(pltpu.make_async_copy(hbm, buf, in_sem.at[4 * nblk + n]))

    last = nblk - 1
    barrier = pltpu.get_barrier_semaphore()
    extra[0].start()
    for b in (last - 1, last):
        load(1, b).start()
        load(2, b).start()
    signal(barrier, at_chip(z + 1))
    signal(barrier, at_chip(z - 1))

    @pl.when(has_prev)
    def _():
        signal(barrier, prev)

    @pl.when(has_next)
    def _():
        signal(barrier, nxt)

    load(0, 0).start()
    load(3, 0).start()
    extra[1].start()
    extra[2].start()
    extra[3].start()
    load(0, last).start()
    for b in range(nblk):
        for array in range(4):
            if not (array in (1, 2) and b >= last - 1) and not (array in (0, 3) and b == 0) and not (array == 0 and b == last):
                load(array, b).start()
    extra[4].start()

    @pl.when(jnp.logical_not(has_prev))
    def _():
        for buf in (qb, kb, vb):
            buf[0:ROWS, :] = jnp.zeros((ROWS, width), BF16)
        xz[0, 0 : 2 * BLK, :] = jnp.zeros((2 * BLK, width), BF16)

    @pl.when(jnp.logical_not(has_next))
    def _():
        nq[...] = jnp.zeros_like(nq)
        ny[...] = jnp.zeros_like(ny)
        xg[nblk, 0 : 2 * BLK, :] = jnp.zeros((2 * BLK, width), BF16)
        nx[...] = jnp.zeros_like(nx)

    def delayed(now, before):
        cat = jnp.concatenate([before.astype(F32)[8:], now.astype(F32)], 0)
        return cat[8:], pltpu.roll(cat, 1, 0)[8:], pltpu.roll(cat, 2, 0)[8:]

    def feat(now, before, which):
        own, one, two = delayed(now, before)
        return sf[which, 0:1, :] * own + sf[which, 1:2, :] * one + sf[which, 2:3, :] * two

    def put(ref, b, n, value):
        high = value.astype(BF16)
        low = (value - high.astype(F32)).astype(BF16)
        ref[b, pl.ds(n, ROWS), :] = high
        ref[b, pl.ds(BLK + n, ROWS), :] = low
        ref[b, pl.ds(2 * BLK + n, ROWS), :] = high

    def z_chunk(b, n):
        row = b * BLK + n
        kk = feat(kb[pl.ds(row + ROWS, ROWS), :], kb[pl.ds(row, ROWS), :], 1)
        vv = feat(vb[pl.ds(row + ROWS, ROWS), :], vb[pl.ds(row, ROWS), :], 2)
        kf[pl.ds(row, ROWS), :] = kk
        vf[pl.ds(row, ROWS), :] = vv
        put(xz, b + 1, n, kk * vv)

    def g_chunk(b, n):
        row = b * BLK + n
        qq = feat(qb[pl.ds(row + ROWS, ROWS), :], qb[pl.ds(row, ROWS), :], 0)
        put(xg, b, n, yb[pl.ds(row, ROWS), :].astype(F32) * qq)

    def chunks(body, first, stop):
        def step(i, carry):
            body(pl.multiple_of(i * ROWS, ROWS))
            return carry

        lax.fori_loop(first, stop, step, 0)

    per = BLK // ROWS
    extra[0].wait()
    for b in (last - 1, last):
        load(1, b).wait()
        load(2, b).wait()
    chunks(lambda n: z_chunk(last, n), 0, per)
    load(0, 0).wait()
    load(3, 0).wait()
    chunks(lambda n: g_chunk(0, n), 1, per)
    load(0, last).wait()

    count = 2 + has_prev.astype(jnp.int32) + has_next.astype(jnp.int32)
    pl.semaphore_wait(barrier, count)
    tail = pl.ds(length, ROWS)
    to_next = [remote(buf.at[tail], buf.at[pl.ds(0, ROWS)], n, nxt) for n, buf in enumerate((qb, kb, vb))]
    z_halo = remote(xz.at[nblk, pl.ds(0, 2 * BLK)], xz.at[0, pl.ds(0, 2 * BLK)], 3, nxt)
    to_prev = [
        remote(qb.at[pl.ds(ROWS, ROWS)], nq, 4, prev),
        remote(yb.at[pl.ds(0, ROWS)], ny, 5, prev),
    ]
    g_halo = [
        remote(xg.at[0, pl.ds(h * BLK + ROWS, BLK - ROWS)], xg.at[nblk, pl.ds(h * BLK + ROWS, BLK - ROWS)], 6 + h, prev)
        for h in range(2)
    ]

    @pl.when(has_next)
    def _():
        for copy in to_next:
            copy.start()
        z_halo.start()

    @pl.when(has_prev)
    def _():
        for copy in to_prev + g_halo:
            copy.start()

    steps = []
    radius = 1
    while radius < chips // 2:
        steps.append(radius)
        radius *= 2

    def tell(n):
        if n < len(steps):
            signal(known.at[n], at_chip(z + steps[n]))
            signal(known.at[n], at_chip(z - steps[n]))

    def learn(n):
        if n < len(steps):
            pl.semaphore_wait(known.at[n], 2)

    tell(0)

    extra[1].wait()
    extra[2].wait()

    def h_chunk(n):
        put(xh, 0, n, lf[pl.ds(n, ROWS), :])

    chunks(h_chunk, 1, per)
    first = lf[0:ROWS, :]
    at_zero = lax.broadcasted_iota(jnp.int32, (ROWS, width), 0) == 0
    put(xh, 0, 0, jnp.where(at_zero, first + sg[...], first))
    extra[3].wait()

    def dft(x, b, out, o):
        for lane in range(0, width, 256):
            cols = slice(lane, lane + 256)
            out[o, :, cols] = jnp.dot(fwd[...], x[b, :, cols], preferred_element_type=F32)

    def inverse(x, b):
        return jnp.dot(inv[...], x[b], preferred_element_type=F32)

    dft(xh, 0, hs, 0)
    for b in range(last):
        load(1, b).wait() if b < last - 1 else None
        load(2, b).wait() if b < last - 1 else None
        chunks(functools.partial(z_chunk, b), 1 if b == 0 else 0, per)
    for b in range(1, nblk):
        load(0, b).wait() if b < last else None
        load(3, b).wait()
        chunks(functools.partial(g_chunk, b), 0, per)
    learn(0)
    tell(1)
    for b in range(1, nblk):
        dft(xz, b + 1, zs, b + 1)
        dft(xg, b, gs, b)
    learn(1)
    tell(2)

    @pl.when(has_prev)
    def _():
        for copy in to_next:
            copy.wait_recv()

    z_chunk(0, 0)
    g_chunk(0, 0)
    dft(xz, 1, zs, 1)
    dft(xg, 0, gs, 0)
    extra[4].wait()

    def put_spectrum(ref, b, k, lanes, real, imag):
        for off, value in ((0, real), (BLK, imag)):
            high = value.astype(BF16)
            low = (value - high.astype(F32)).astype(BF16)
            ref[b, pl.ds(off + k, ROWS), lanes] = high
            ref[b, pl.ds(2 * BLK + off + k, ROWS), lanes] = low
            ref[b, pl.ds(4 * BLK + off + k, ROWS), lanes] = high

    def by_frequency(body):
        for sign, start in ((1.0, 0), (-1.0, BLK // 2)):
            for lane in range(0, width, 256):

                def step(i, carry, sign=sign, start=start, lane=lane):
                    body(pl.multiple_of(start + i * ROWS, ROWS), slice(lane, lane + 256), sign)
                    return carry

                lax.fori_loop(0, BLK // 2 // ROWS, step, 0)

    def add(a, sign, b):
        return a + b if sign > 0 else a - b

    def z_spectrum(b, start, k, lanes, sign):
        re, im = pl.ds(k, ROWS), pl.ds(BLK + k, ROWS)
        vr = add(zs[b + 1, re, lanes], -sign, zs[b, im, lanes])
        vi = add(zs[b + 1, im, lanes], sign, zs[b, re, lanes])
        hr, hi = hs[0, re, lanes], hs[0, im, lanes]
        put_spectrum(xs, b, k, lanes, hr * vr - hi * vi, hr * vi + hi * vr)
        gr, gi = gs[b, re, lanes], gs[b, im, lanes]
        lr, li = gr * vr + gi * vi, gi * vr - gr * vi
        if not start:
            lr, li = gl_f[re, lanes] + lr, gl_f[im, lanes] + li
        return lr, li

    def z_stage(b, start, final):
        def body(k, lanes, sign):
            lr, li = z_spectrum(b, start, k, lanes, sign)
            if final:
                put_spectrum(xgl, 0, k, lanes, lr, li)
            else:
                gl_f[pl.ds(k, ROWS), lanes] = lr
                gl_f[pl.ds(BLK + k, ROWS), lanes] = li

        by_frequency(body)

    def g_stage(b):
        def body(k, lanes, sign):
            re, im = pl.ds(k, ROWS), pl.ds(BLK + k, ROWS)
            ur = add(gs[b, re, lanes], sign, gs[b + 1, im, lanes])
            ui = add(gs[b, im, lanes], -sign, gs[b + 1, re, lanes])
            hr, hi = hs[0, re, lanes], hs[0, im, lanes]
            put_spectrum(xu, b, k, lanes, hr * ur + hi * ui, hr * ui - hi * ur)

        by_frequency(body)

    def out_rows(b):
        return slice(b * BLK, (b + 1) * BLK)

    for b in range(1, nblk):
        z_stage(b, b == 1, False)
        s_t[out_rows(b), :] = inverse(xs, b)
    for b in range(last):
        g_stage(b)
        gz_t[out_rows(b), :] = inverse(xu, b)

    @pl.when(has_prev)
    def _():
        z_halo.wait_recv()

    xz[0, 2 * BLK :, :] = xz[0, 0:BLK, :]
    dft(xz, 0, zs, 0)
    z_stage(0, False, True)
    gl = inverse(xgl, 0)
    share = BLK // total
    for i in range(total):
        glt[i % 2, i // 2] = gl[share * i : share * (i + 1), :]
    small[9:10, :] = gl[0:1, :]
    to_partner = remote(glt.at[1 - c], gl_in, 8, partner)
    to_partner.start()

    s_t[out_rows(0), :] = inverse(xs, 0)
    row = lax.broadcasted_iota(jnp.int32, (8, width), 0)
    gq8 = yb[0:ROWS, :].astype(F32)[0:8] * s_t[0:8, :]
    gk8 = gz_t[0:8, :] * vf[0:8, :]
    gv8 = gz_t[0:8, :] * kf[0:8, :]
    mine3[...] = jnp.where(row < 2, gq8, jnp.where(row < 4, pltpu.roll(gk8, 2, 0), pltpu.roll(gv8, 4, 0)))
    firsts = remote(mine3, nx, 9, prev)

    @pl.when(has_prev)
    def _():
        firsts.start()

    learn(2)
    to_partner.wait_recv()
    racc[...] = glt[c] + gl_in[...]
    scatter = []
    order = sorted(range(1, chips), key=lambda d: (-min(d, chips - d), d))
    for d in order:
        chip = lax.rem(z + d, chips)
        copy = remote(racc.at[chip], rs_in.at[d], 16 + d, at_chip(chip))
        copy.start()
        scatter.append(copy)

    @pl.when(has_next)
    def _():
        for copy in to_prev + g_halo:
            copy.wait_recv()

    put(xg, nblk, 0, ny[...].astype(F32) * feat(nq[...], qb[tail, :], 0))
    xg[nblk, 2 * BLK + ROWS :, :] = xg[nblk, ROWS:BLK, :]
    dft(xg, nblk, gs, nblk)
    g_stage(last)
    gz_t[out_rows(last), :] = inverse(xu, last)

    def q_rows(row, n):
        return yb[pl.ds(row, ROWS), :].astype(F32)[0:n] * s_t[pl.ds(row, n), :]

    def k_rows(row, n):
        return gz_t[pl.ds(row, n), :] * vf[pl.ds(row, n), :]

    def v_rows(row, n):
        return gz_t[pl.ds(row, n), :] * kf[pl.ds(row, n), :]

    def back(which, rows_of, raw, out, row, after, sums):
        grad = rows_of(row, ROWS)
        cat = jnp.concatenate([grad, rows_of(row + ROWS, 8) if after is None else after], 0)
        one = pltpu.roll(cat, ROWS + 7, 0)[0:ROWS]
        two = pltpu.roll(cat, ROWS + 6, 0)[0:ROWS]
        value = sf[which, 0:1, :] * grad + sf[which, 1:2, :] * one + sf[which, 2:3, :] * two
        out[pl.ds(row, ROWS), :] = value.astype(BF16)
        parts = delayed(raw[pl.ds(row + ROWS, ROWS), :], raw[pl.ds(row, ROWS), :])
        products = [grad * part for part in parts]
        return tuple(s + p[0:8] + p[8:16] for s, p in zip(sums, products))

    kinds = ((0, q_rows, qb, oq), (1, k_rows, kb, ok), (2, v_rows, vb, ov))
    sums = []
    for which, rows_of, raw, out in kinds:

        def step(i, carry, which=which, rows_of=rows_of, raw=raw, out=out):
            return back(which, rows_of, raw, out, pl.multiple_of(i * ROWS, ROWS), None, carry)

        zero = jnp.zeros((8, width), F32)
        sums.append(lax.fori_loop(0, length // ROWS - 1, step, (zero, zero, zero)))

    @pl.when(has_next)
    def _():
        firsts.wait_recv()

    after = nx[...]
    afters = (after, pltpu.roll(after, 6, 0), pltpu.roll(after, 4, 0))
    for (which, rows_of, raw, out), carry, rows in zip(kinds, sums, afters):
        carry = back(which, rows_of, raw, out, length - ROWS, rows, carry)
        for i in range(3):
            small[3 * which + i : 3 * which + i + 1, :] = jnp.sum(carry[i], axis=0, keepdims=True)

    row = lax.broadcasted_iota(jnp.int32, (8, 128), 0)
    for h in range(2):
        lane = 256 * h
        half[h, 0] = small[0:8, lane : lane + 128]
        half[h, 1] = small[0:8, lane + 128 : lane + 256]
        half[h, 2] = jnp.where(
            row < 2,
            small[8:16, lane : lane + 128],
            jnp.where(row < 4, pltpu.roll(small[8:16, lane + 128 : lane + 256], 2, 0), 0.0),
        )
    halves = remote(half.at[1 - c], half_in, 10, partner)
    halves.start()
    halves.wait_recv()
    ar[z] = half[c] + half_in[...]
    spread = []
    for d in order:
        copy = remote(ar.at[z], ar.at[z], 16 + chips + d, at_chip(z + d))
        copy.start()
        spread.append(copy)

    for copy in scatter:
        copy.wait_recv()
    taps = racc[z]
    for d in range(1, chips):
        taps = taps + rs_in[d]
    ofilt[...] = taps

    for copy in spread:
        copy.wait_recv()
    whole = ar[0]
    for chip in range(1, chips):
        whole = whole + ar[chip]
    fin[c] = whole
    final = remote(fin.at[c], fin.at[c], 11, partner)
    final.start()
    final.wait_recv()
    for h in range(2):
        for j in range(2):
            cols = slice(256 * h + 128 * j, 256 * h + 128 * (j + 1))
            for i in range(8):
                otaps[i // 3, i % 3 : i % 3 + 1, cols] = fin[h, j, i : i + 1, :]
            otaps[2, 2:3, cols] = fin[h, 2, 2 * j : 2 * j + 1, :]
            ogain[0:1, cols] = fin[h, 2, 2 * j + 1 : 2 * j + 2, :]

    @pl.when(has_next)
    def _():
        for copy in to_next:
            copy.wait_send()
        z_halo.wait_send()

    @pl.when(has_prev)
    def _():
        for copy in to_prev + g_halo + [firsts]:
            copy.wait_send()

    for copy in [to_partner, halves, final] + scatter + spread:
        copy.wait_send()


def put_out(*refs):
    sem = refs[-1]
    copies = [pltpu.make_async_copy(refs[n], refs[n + 6], sem.at[n]) for n in range(6)]
    for copy in copies:
        copy.start()
    for copy in copies:
        copy.wait()


def body(fwd, inv, chips, input_q, input_k, input_v, grad_out, short_filters, long_filter, skip_gain):
    length, width = input_q.shape
    nblk = length // BLK
    reach = length + ROWS
    hbm = pl.BlockSpec(memory_space=pltpu.HBM)
    vmem = pl.BlockSpec(memory_space=pltpu.VMEM)
    scratch = [
        *(pltpu.VMEM((reach, width), BF16) for _ in range(3)),
        pltpu.VMEM((length, width), BF16),
        pltpu.VMEM((ROWS, width), BF16),
        pltpu.VMEM((ROWS, width), BF16),
        pltpu.VMEM(short_filters.shape, F32),
        pltpu.VMEM(long_filter.shape, F32),
        pltpu.VMEM((1, width), F32),
        pltpu.VMEM(fwd.shape, BF16),
        pltpu.VMEM(inv.shape, BF16),
        *(pltpu.VMEM((length, width), F32) for _ in range(4)),
        pltpu.VMEM((nblk + 1, 3 * BLK, width), BF16),
        pltpu.VMEM((nblk + 1, 3 * BLK, width), BF16),
        pltpu.VMEM((1, 3 * BLK, width), BF16),
        pltpu.VMEM((nblk + 1, 2 * BLK, width), F32),
        pltpu.VMEM((nblk + 1, 2 * BLK, width), F32),
        pltpu.VMEM((1, 2 * BLK, width), F32),
        pltpu.VMEM((nblk, 6 * BLK, width), BF16),
        pltpu.VMEM((nblk, 6 * BLK, width), BF16),
        pltpu.VMEM((2 * BLK, width), F32),
        pltpu.VMEM((1, 6 * BLK, width), BF16),
        pltpu.VMEM((8, width), F32),
        pltpu.VMEM((8, width), F32),
        pltpu.VMEM((2, chips, BLK // (2 * chips), width), F32),
        pltpu.VMEM((chips, BLK // (2 * chips), width), F32),
        pltpu.VMEM((chips, BLK // (2 * chips), width), F32),
        pltpu.VMEM((chips, BLK // (2 * chips), width), F32),
        pltpu.VMEM((16, width), F32),
        pltpu.VMEM((2, 3, 8, 128), F32),
        pltpu.VMEM((3, 8, 128), F32),
        pltpu.VMEM((chips, 3, 8, 128), F32),
        pltpu.VMEM((2, 3, 8, 128), F32),
        pltpu.SemaphoreType.DMA((4 * nblk + 5,)),
        pltpu.SemaphoreType.DMA((16 + 2 * chips,)),
        pltpu.SemaphoreType.DMA((16 + 2 * chips,)),
        pltpu.SemaphoreType.REGULAR((3,)),
    ]
    operands = (input_q, input_k, input_v, grad_out, short_filters, long_filter, skip_gain[None], fwd, inv)
    outs = pl.pallas_call(
        functools.partial(kernel, chips),
        out_shape=(
            *(pltpu.VMEM((length, width), BF16) for _ in range(3)),
            pltpu.VMEM((BLK // (2 * chips), width), F32),
            pltpu.VMEM(short_filters.shape, F32),
            pltpu.VMEM((1, width), F32),
        ),
        in_specs=[hbm] * 9,
        out_specs=(vmem,) * 6,
        scratch_shapes=scratch,
        compiler_params=pltpu.CompilerParams(
            collective_id=0, has_side_effects=True, vmem_limit_bytes=48 * 1024 * 1024
        ),
        name="hyena_backward",
    )(*(pltpu.with_memory_space_constraint(a, pltpu.HBM) for a in operands))
    done = pl.pallas_call(
        put_out,
        out_shape=tuple(jax.ShapeDtypeStruct(o.shape, o.dtype) for o in outs),
        in_specs=[vmem] * 6,
        out_specs=(hbm,) * 6,
        scratch_shapes=[pltpu.SemaphoreType.DMA((6,))],
        compiler_params=pltpu.CompilerParams(vmem_limit_bytes=1 << 20),
        name="put_out",
    )(*outs)
    return (*done[:5], done[5][0])


def solution(mesh):
    chips = mesh.shape["seq"] // 2
    fwd, inv = tables()

    def run(*arrays):
        return body(jnp.asarray(fwd), jnp.asarray(inv), chips, *arrays)

    return jax.shard_map(
        run,
        mesh=mesh,
        in_specs=(
            P("seq", "ch"),
            P("seq", "ch"),
            P("seq", "ch"),
            P("seq", "ch"),
            P(None, None, "ch"),
            P(None, "ch"),
            P("ch"),
        ),
        out_specs=(
            P("seq", "ch"),
            P("seq", "ch"),
            P("seq", "ch"),
            P("seq", "ch"),
            P(None, None, "ch"),
            P("ch"),
        ),
        check_vma=False,
    )
```

```python
import functools

import jax
import jax.numpy as jnp
import ml_dtypes
import numpy as np
from jax import lax
from jax.experimental import pallas as pl
from jax.experimental.pallas import tpu as pltpu
from jax.sharding import PartitionSpec as P

F32, BF16 = jnp.float32, jnp.bfloat16
BLK = 128
ROWS = 16
PAD = 8
LANES = 128


def tables():
    order = np.concatenate([np.arange(0, BLK, 2), np.arange(1, BLK, 2)])
    angle = np.outer(np.pi * (2 * order + 1) / (2 * BLK), np.arange(BLK))
    full = np.concatenate([np.cos(angle), -np.sin(angle)], 0)
    high = full.astype(ml_dtypes.bfloat16).astype(np.float64)
    low = full - high
    fwd = np.concatenate([high, high, low], 1)
    inv = np.concatenate([high.T, high.T, low.T], 1) / BLK
    return fwd.astype(ml_dtypes.bfloat16), inv.astype(ml_dtypes.bfloat16)


def kernel(
    chips,
    q_hbm, k_hbm, v_hbm, y_hbm, sf_hbm, lf_hbm, sg_hbm, fwd_hbm, inv_hbm,
    oq, ok, ov, ofilt, otaps, ogain,
    qb, kb, vb, yb, hq, hk, hv, nq, ny, sf, lf, sg, fwd, inv,
    rq, rk, rv, rn, kf, vf, gq, gk, gv, xz, xg, xh, zs, gs, hs, xs, xu, gl_f, xgl,
    mine3, nx, glt, gl_in, racc, rs_in, taps, half, half_in, near, far, fin,
    in_sem, send, recv, known,
):
    length = q_hbm.shape[0]
    width = q_hbm.shape[1]
    tiles = width // LANES
    nblk = length // BLK
    last = nblk - 1
    me = lax.axis_index("seq")
    total = 2 * chips
    z, c = me // 2, lax.rem(me, 2)
    has_prev, has_next = me > 0, me < total - 1
    prev, nxt = me - 1, me + 1
    partner = me + 1 - 2 * c

    def at_chip(chip):
        return lax.rem(chip + chips, chips) * 2 + c

    def remote(src, dst, slot, device):
        return pltpu.make_async_remote_copy(
            src_ref=src, dst_ref=dst, send_sem=send.at[slot], recv_sem=recv.at[slot],
            device_id={"seq": device}, device_id_type=pl.DeviceIdType.MESH,
        )

    def signal(sem, device):
        pl.semaphore_signal(sem, 1, device_id={"seq": device}, device_id_type=pl.DeviceIdType.MESH)

    barrier = pltpu.get_barrier_semaphore()
    signal(barrier, at_chip(z + 1))
    signal(barrier, at_chip(z - 1))

    @pl.when(has_prev)
    def _():
        signal(barrier, prev)

    @pl.when(has_next)
    def _():
        signal(barrier, nxt)

    def load(array, b):
        hbm, buf = ((q_hbm, qb), (k_hbm, kb), (v_hbm, vb), (y_hbm, yb))[array]
        rows = pl.ds(b * BLK, BLK)
        return pltpu.make_async_copy(hbm.at[rows], buf.at[rows], in_sem.at[array * nblk + b])

    extra = []
    for n, (hbm, buf) in enumerate(((sf_hbm, sf), (lf_hbm, lf), (sg_hbm, sg), (fwd_hbm, fwd), (inv_hbm, inv))):
        extra.append(pltpu.make_async_copy(hbm, buf, in_sem.at[4 * nblk + n]))

    extra[0].start()
    early = [(1, last - 1), (2, last - 1), (1, last), (2, last), (0, 0), (3, 0), (0, last)]
    for key in early:
        load(*key).start()
    for copy in extra[1:4]:
        copy.start()
    for b in range(nblk):
        for array in (1, 2, 0, 3):
            if (array, b) not in early:
                load(array, b).start()
    extra[4].start()
    waited = set()

    def ready(*keys):
        for key in keys:
            if key not in waited:
                waited.add(key)
                load(*key).wait()

    @pl.when(jnp.logical_not(has_prev))
    def _():
        for buf in (hq, hk, hv):
            buf[...] = jnp.zeros_like(buf)
        xz[0, 0 : 2 * BLK, :] = jnp.zeros((2 * BLK, width), BF16)

    @pl.when(jnp.logical_not(has_next))
    def _():
        nq[...] = jnp.zeros_like(nq)
        ny[...] = jnp.zeros_like(ny)
        xg[nblk, 0 : 2 * BLK, :] = jnp.zeros((2 * BLK, width), BF16)
        nx[...] = jnp.zeros_like(nx)

    for h in range(2):
        half[h, 2] = jnp.zeros((8, LANES), F32)

    def by_tile(body):
        for j in range(tiles):
            body(j, slice(j * LANES, (j + 1) * LANES))

    def weights(which, lanes):
        return [sf[which, i : i + 1, lanes] for i in range(3)]

    def widen(buf, raw, j, lanes, r0, r1):
        raw[j, PAD + r0 : PAD + r1, :] = buf[r0:r1, lanes].astype(F32)

    def feat(raw, j, w, r0, r1):
        return (
            w[0] * raw[j, PAD + r0 : PAD + r1, :]
            + w[1] * raw[j, PAD + r0 - 1 : PAD + r1 - 1, :]
            + w[2] * raw[j, PAD + r0 - 2 : PAD + r1 - 2, :]
        )

    def put(ref, b, n, lanes, value):
        size = value.shape[0]
        high = value.astype(BF16)
        low = (value - high.astype(F32)).astype(BF16)
        ref[b, n : n + size, lanes] = high
        ref[b, BLK + n : BLK + n + size, lanes] = low
        ref[b, 2 * BLK + n : 2 * BLK + n + size, lanes] = high

    def z_rows(b, n0, n1, wide=True):
        def body(j, lanes):
            wk, wv = weights(1, lanes), weights(2, lanes)
            if wide:
                widen(kb, rk, j, lanes, b * BLK + n0, b * BLK + n1)
                widen(vb, rv, j, lanes, b * BLK + n0, b * BLK + n1)
            for n in range(n0, n1, ROWS):
                r0 = b * BLK + n
                kk, vv = feat(rk, j, wk, r0, r0 + ROWS), feat(rv, j, wv, r0, r0 + ROWS)
                kf[j, r0 : r0 + ROWS, :] = kk
                vf[j, r0 : r0 + ROWS, :] = vv
                put(xz, b + 1, n, lanes, kk * vv)

        by_tile(body)

    def g_rows(b, n0, n1, wide=True):
        def body(j, lanes):
            wq = weights(0, lanes)
            if wide:
                widen(qb, rq, j, lanes, b * BLK + n0, b * BLK + n1)
            for n in range(n0, n1, ROWS):
                r0 = b * BLK + n
                put(xg, b, n, lanes, yb[r0 : r0 + ROWS, lanes].astype(F32) * feat(rq, j, wq, r0, r0 + ROWS))

        by_tile(body)

    extra[0].wait()
    ready((1, last - 1), (2, last - 1), (1, last), (2, last))

    def before_last(j, lanes):
        widen(kb, rk, j, lanes, last * BLK - ROWS, last * BLK)
        widen(vb, rv, j, lanes, last * BLK - ROWS, last * BLK)

    by_tile(before_last)
    z_rows(last, 0, BLK)
    ready((0, 0), (3, 0))
    by_tile(lambda j, lanes: widen(qb, rq, j, lanes, 0, ROWS))
    g_rows(0, ROWS, BLK)
    ready((0, last))

    count = 2 + has_prev.astype(jnp.int32) + has_next.astype(jnp.int32)
    pl.semaphore_wait(barrier, count)
    tail = pl.ds(length - PAD, PAD)
    to_next = [remote(buf.at[tail], hist, n, nxt) for n, (buf, hist) in enumerate(((qb, hq), (kb, hk), (vb, hv)))]
    z_halo = remote(xz.at[nblk, pl.ds(0, 2 * BLK)], xz.at[0, pl.ds(0, 2 * BLK)], 3, nxt)
    head = pl.ds(0, ROWS)
    to_prev = [remote(qb.at[head], nq, 4, prev), remote(yb.at[head], ny, 5, prev)]
    g_halo = [
        remote(xg.at[0, pl.ds(h * BLK + ROWS, BLK - ROWS)], xg.at[nblk, pl.ds(h * BLK + ROWS, BLK - ROWS)], 6 + h, prev)
        for h in range(2)
    ]

    @pl.when(has_next)
    def _():
        for copy in to_next:
            copy.start()
        z_halo.start()

    @pl.when(has_prev)
    def _():
        for copy in to_prev + g_halo:
            copy.start()

    steps = []
    radius = 1
    while radius < chips // 2:
        steps.append(radius)
        radius *= 2

    def tell(n):
        if n < len(steps):
            signal(known.at[n], at_chip(z + steps[n]))
            signal(known.at[n], at_chip(z - steps[n]))

    def learn(n):
        if n < len(steps):
            pl.semaphore_wait(known.at[n], 2)

    tell(0)

    for b in range(nblk):
        ready((0, b), (1, b), (2, b), (3, b))
    for copy in extra[1:]:
        copy.wait()
    for b in range(last):
        if b == 0:
            by_tile(lambda j, lanes: (widen(kb, rk, j, lanes, 0, ROWS), widen(vb, rv, j, lanes, 0, ROWS)))
        z_rows(b, ROWS if b == 0 else 0, BLK)
    for b in range(1, nblk):
        g_rows(b, 0, BLK)


    def filter_rows(j, lanes):
        first = lf[0:ROWS, lanes]
        at_zero = lax.broadcasted_iota(jnp.int32, (ROWS, LANES), 0) == 0
        put(xh, 0, 0, lanes, jnp.where(at_zero, first + sg[:, lanes], first))
        put(xh, 0, ROWS, lanes, lf[ROWS:BLK, lanes])

    by_tile(filter_rows)

    def dft(x, b, out, o):
        for lane in range(0, width, 256):
            cols = slice(lane, lane + 256)
            out[o, :, cols] = jnp.dot(fwd[...], x[b, :, cols], preferred_element_type=F32)

    dft(xh, 0, hs, 0)
    for b in range(1, nblk):
        dft(xz, b + 1, zs, b + 1)
        dft(xg, b, gs, b)
    learn(0)
    tell(1)
    @pl.when(has_prev)
    def _():
        for copy in to_next:
            copy.wait_recv()

    def history(j, lanes):
        for raw, hist in ((rq, hq), (rk, hk), (rv, hv)):
            raw[j, 0:PAD, :] = hist[:, lanes].astype(F32)

    by_tile(history)
    z_rows(0, 0, ROWS, False)
    g_rows(0, 0, ROWS, False)
    dft(xz, 1, zs, 1)
    dft(xg, 0, gs, 0)

    def put_spectrum(ref, b, k, lanes, real, imag):
        for off, value in ((0, real), (BLK, imag)):
            high = value.astype(BF16)
            low = (value - high.astype(F32)).astype(BF16)
            ref[b, off + k : off + k + ROWS, lanes] = high
            ref[b, 2 * BLK + off + k : 2 * BLK + off + k + ROWS, lanes] = low
            ref[b, 4 * BLK + off + k : 4 * BLK + off + k + ROWS, lanes] = high

    def add(a, sign, b):
        return a + b if sign > 0 else a - b

    def frequencies():
        for k in range(0, BLK, ROWS):
            yield k, slice(k, k + ROWS), slice(BLK + k, BLK + k + ROWS), 1 if k < BLK // 2 else -1

    def z_stage(blocks, final):
        def body(j, lanes):
            for k, re, im, sign in frequencies():
                hr, hi = hs[0, re, lanes], hs[0, im, lanes]
                lr = li = None
                if final:
                    lr, li = gl_f[re, lanes], gl_f[im, lanes]
                for b in blocks:
                    vr = add(zs[b + 1, re, lanes], -sign, zs[b, im, lanes])
                    vi = add(zs[b + 1, im, lanes], sign, zs[b, re, lanes])
                    gr, gi = gs[b, re, lanes], gs[b, im, lanes]
                    pr, pi = gr * vr + gi * vi, gi * vr - gr * vi
                    lr, li = (pr, pi) if lr is None else (lr + pr, li + pi)
                    put_spectrum(xs, b, k, lanes, hr * vr - hi * vi, hr * vi + hi * vr)
                if final:
                    put_spectrum(xgl, 0, k, lanes, lr, li)
                else:
                    gl_f[re, lanes] = lr
                    gl_f[im, lanes] = li

        by_tile(body)

    def g_stage(blocks):
        def body(j, lanes):
            for k, re, im, sign in frequencies():
                hr, hi = hs[0, re, lanes], hs[0, im, lanes]
                for b in blocks:
                    ur = add(gs[b, re, lanes], sign, gs[b + 1, im, lanes])
                    ui = add(gs[b, im, lanes], -sign, gs[b + 1, re, lanes])
                    put_spectrum(xu, b, k, lanes, hr * ur + hi * ui, hr * ui - hi * ur)

        by_tile(body)

    def inverse(x, b, use):
        for lane in range(0, width, 256):
            value = jnp.dot(inv[...], x[b, :, lane : lane + 256], preferred_element_type=F32)
            for part in range(0, 256, LANES):
                use(b, (lane + part) // LANES, value[:, part : part + LANES])

    def use_s(b, j, value):
        rows = slice(b * BLK, (b + 1) * BLK)
        gq[j, rows, :] = value * yb[rows, LANES * j : LANES * (j + 1)].astype(F32)

    def use_gz(b, j, value):
        rows = slice(b * BLK, (b + 1) * BLK)
        gk[j, rows, :] = value * vf[j, rows, :]
        gv[j, rows, :] = value * kf[j, rows, :]

    kinds = ((gq, rq, oq), (gk, rk, ok), (gv, rv, ov))

    def finish(which, r0, r1, fresh=False, write=True, count=True):
        grad, raw, out = kinds[which]

        def body(j, lanes):
            w = weights(which, lanes)
            sums = [None if fresh else taps[3 * which + i, j] for i in range(3)] if count else None
            for r in range(r0, r1, ROWS):
                own = grad[j, r : r + ROWS, :]
                if write:
                    one, two = grad[j, r + 1 : r + 1 + ROWS, :], grad[j, r + 2 : r + 2 + ROWS, :]
                    out[r : r + ROWS, lanes] = (w[0] * own + w[1] * one + w[2] * two).astype(BF16)
                if count:
                    for i in range(3):
                        product = own * raw[j, PAD + r - i : PAD + r - i + ROWS, :]
                        product = product[0:8] + product[8:16]
                        sums[i] = product if sums[i] is None else sums[i] + product
            if count:
                for i in range(3):
                    taps[3 * which + i, j] = sums[i]

        by_tile(body)

    z_stage(range(1, nblk), False)
    g_stage(range(last))
    for b in range(1, nblk):
        inverse(xs, b, use_s)
    for b in range(last):
        inverse(xu, b, use_gz)
    finish(0, BLK, length - ROWS, True)
    finish(0, length - ROWS, length, write=False)
    for which in (1, 2):
        finish(which, 0, last * BLK - ROWS, True)

    learn(1)
    tell(2)

    @pl.when(has_prev)
    def _():
        z_halo.wait_recv()

    @pl.when(has_next)
    def _():
        for copy in to_prev + g_halo:
            copy.wait_recv()

    share = BLK // total

    def next_rows(j, lanes):
        w = weights(0, lanes)
        rn[j, 0:PAD, :] = rq[j, length : length + PAD, :]
        rn[j, PAD : PAD + ROWS, :] = nq[:, lanes].astype(F32)
        put(xg, nblk, 0, lanes, ny[:, lanes].astype(F32) * feat(rn, j, w, 0, ROWS))

    def use_gl(b, j, value):
        cols = slice(LANES * j, LANES * (j + 1))
        for i in range(total):
            glt[i % 2, i // 2, :, cols] = value[share * i : share * (i + 1), :]
        half[j // 2, 2, 2 * (j % 2) + 1 : 2 * (j % 2) + 2, :] = value[0:1, :]

    xz[0, 2 * BLK :, :] = xz[0, 0:BLK, :]
    by_tile(next_rows)
    xg[nblk, 2 * BLK + ROWS :, :] = xg[nblk, ROWS:BLK, :]
    dft(xz, 0, zs, 0)
    dft(xg, nblk, gs, nblk)
    z_stage((0,), True)
    g_stage((last,))
    inverse(xs, 0, use_s)
    inverse(xgl, 0, use_gl)
    inverse(xu, last, use_gz)
    row = lax.broadcasted_iota(jnp.int32, (8, LANES), 0)
    for j in range(tiles):
        second, third = pltpu.roll(gk[j, 0:8, :], 2, 0), pltpu.roll(gv[j, 0:8, :], 4, 0)
        mine3[j] = jnp.where(row < 2, gq[j, 0:8, :], jnp.where(row < 4, second, third))
    to_partner = remote(glt.at[1 - c], gl_in, 8, partner)
    to_partner.start()
    finish(0, 0, BLK)
    for which in (1, 2):
        finish(which, last * BLK - ROWS, length - ROWS)
        finish(which, length - ROWS, length, write=False)
    for j in range(tiles):
        h, jj = j // 2, j % 2
        for n in range(9):
            total_n = jnp.sum(taps[n, j], axis=0, keepdims=True)
            if n < 8:
                half[h, jj, n : n + 1, :] = total_n
            else:
                half[h, 2, 2 * jj : 2 * jj + 1, :] = total_n
    halves = remote(half.at[1 - c], half_in, 10, partner)
    halves.start()
    firsts = remote(mine3, nx, 9, prev)

    @pl.when(has_prev)
    def _():
        firsts.start()

    to_partner.wait_recv()
    racc[...] = glt[c] + gl_in[...]
    halves.wait_recv()
    group = min(4, chips)
    base = z // group * group
    place = z - base
    near[place] = half[c] + half_in[...]
    close = []
    for d in range(1, group):
        copy = remote(near.at[place], near.at[place], 16 + chips + d, at_chip(base + lax.rem(place + d, group)))
        copy.start()
        close.append(copy)
    learn(2)
    order = sorted(range(1, chips), key=lambda d: (-min(d, chips - d), d))
    cut = 5 if chips == 16 else 1
    scatter = []

    def send_taps(distances):
        for d in distances:
            chip = lax.rem(z + d, chips)
            copy = remote(racc.at[chip], rs_in.at[d], 16 + d, at_chip(chip))
            copy.start()
            scatter.append(copy)

    send_taps(order[:cut])
    @pl.when(has_next)
    def _():
        firsts.wait_recv()

    for j in range(tiles):
        gq[j, length : length + 8, :] = nx[j]
        gk[j, length : length + 8, :] = pltpu.roll(nx[j], 6, 0)
        gv[j, length : length + 8, :] = pltpu.roll(nx[j], 4, 0)
    for which in range(3):
        finish(which, length - ROWS, length, count=False)

    for copy in close:
        copy.wait_recv()
    mine = z // group
    summed = near[0]
    for n in range(1, group):
        summed = summed + near[n]
    far[mine] = summed
    groups = chips // group
    distant = []
    for d in range(1, groups):
        copy = remote(far.at[mine], far.at[mine], 20 + chips + d, at_chip(z + d * group))
        copy.start()
        distant.append(copy)
    send_taps(order[cut:])

    for copy in scatter:
        copy.wait_recv()
    mine_taps = racc[z]
    for d in range(1, chips):
        mine_taps = mine_taps + rs_in[d]
    ofilt[...] = mine_taps

    for copy in distant:
        copy.wait_recv()
    whole = far[0]
    for n in range(1, groups):
        whole = whole + far[n]
    fin[c] = whole
    final = remote(fin.at[c], fin.at[c], 11, partner)
    final.start()
    final.wait_recv()
    for h in range(2):
        for j in range(2):
            cols = slice(256 * h + 128 * j, 256 * h + 128 * (j + 1))
            for i in range(8):
                otaps[i // 3, i % 3 : i % 3 + 1, cols] = fin[h, j, i : i + 1, :]
            otaps[2, 2:3, cols] = fin[h, 2, 2 * j : 2 * j + 1, :]
            ogain[0:1, cols] = fin[h, 2, 2 * j + 1 : 2 * j + 2, :]

    @pl.when(has_next)
    def _():
        for copy in to_next:
            copy.wait_send()
        z_halo.wait_send()

    @pl.when(has_prev)
    def _():
        for copy in to_prev + g_halo + [firsts]:
            copy.wait_send()

    for copy in [to_partner, halves, final] + close + distant + scatter:
        copy.wait_send()


def put_out(*refs):
    sem = refs[-1]
    copies = [pltpu.make_async_copy(refs[n], refs[n + 6], sem.at[n]) for n in range(6)]
    for copy in copies:
        copy.start()
    for copy in copies:
        copy.wait()


def body(fwd, inv, chips, input_q, input_k, input_v, grad_out, short_filters, long_filter, skip_gain):
    length, width = input_q.shape
    nblk = length // BLK
    hbm = pl.BlockSpec(memory_space=pltpu.HBM)
    vmem = pl.BlockSpec(memory_space=pltpu.VMEM)
    tiles = width // LANES
    share = BLK // (2 * chips)
    scratch = [
        *(pltpu.VMEM((length, width), BF16) for _ in range(4)),
        *(pltpu.VMEM((PAD, width), BF16) for _ in range(3)),
        *(pltpu.VMEM((ROWS, width), BF16) for _ in range(2)),
        pltpu.VMEM(short_filters.shape, F32),
        pltpu.VMEM(long_filter.shape, F32),
        pltpu.VMEM((1, width), F32),
        pltpu.VMEM(fwd.shape, BF16),
        pltpu.VMEM(inv.shape, BF16),
        *(pltpu.VMEM((tiles, PAD + length, LANES), F32) for _ in range(3)),
        pltpu.VMEM((tiles, PAD + ROWS, LANES), F32),
        *(pltpu.VMEM((tiles, length, LANES), F32) for _ in range(2)),
        *(pltpu.VMEM((tiles, length + 8, LANES), F32) for _ in range(3)),
        pltpu.VMEM((nblk + 1, 3 * BLK, width), BF16),
        pltpu.VMEM((nblk + 1, 3 * BLK, width), BF16),
        pltpu.VMEM((1, 3 * BLK, width), BF16),
        pltpu.VMEM((nblk + 1, 2 * BLK, width), F32),
        pltpu.VMEM((nblk + 1, 2 * BLK, width), F32),
        pltpu.VMEM((1, 2 * BLK, width), F32),
        pltpu.VMEM((nblk, 6 * BLK, width), BF16),
        pltpu.VMEM((nblk, 6 * BLK, width), BF16),
        pltpu.VMEM((2 * BLK, width), F32),
        pltpu.VMEM((1, 6 * BLK, width), BF16),
        pltpu.VMEM((tiles, 8, LANES), F32),
        pltpu.VMEM((tiles, 8, LANES), F32),
        pltpu.VMEM((2, chips, share, width), F32),
        pltpu.VMEM((chips, share, width), F32),
        pltpu.VMEM((chips, share, width), F32),
        pltpu.VMEM((chips, share, width), F32),
        pltpu.VMEM((9, tiles, 8, LANES), F32),
        pltpu.VMEM((2, 3, 8, LANES), F32),
        pltpu.VMEM((3, 8, LANES), F32),
        pltpu.VMEM((4, 3, 8, LANES), F32),
        pltpu.VMEM((4, 3, 8, LANES), F32),
        pltpu.VMEM((2, 3, 8, LANES), F32),
        pltpu.SemaphoreType.DMA((4 * nblk + 5,)),
        pltpu.SemaphoreType.DMA((32 + chips,)),
        pltpu.SemaphoreType.DMA((32 + chips,)),
        pltpu.SemaphoreType.REGULAR((3,)),
    ]
    operands = (input_q, input_k, input_v, grad_out, short_filters, long_filter, skip_gain[None], fwd, inv)
    outs = pl.pallas_call(
        functools.partial(kernel, chips),
        out_shape=(
            *(pltpu.VMEM((length, width), BF16) for _ in range(3)),
            pltpu.VMEM((BLK // (2 * chips), width), F32),
            pltpu.VMEM(short_filters.shape, F32),
            pltpu.VMEM((1, width), F32),
        ),
        in_specs=[hbm] * 9,
        out_specs=(vmem,) * 6,
        scratch_shapes=scratch,
        compiler_params=pltpu.CompilerParams(
            collective_id=0, has_side_effects=True, vmem_limit_bytes=48 * 1024 * 1024
        ),
        name="hyena_backward",
    )(*(pltpu.with_memory_space_constraint(a, pltpu.HBM) for a in operands))
    done = pl.pallas_call(
        put_out,
        out_shape=tuple(jax.ShapeDtypeStruct(o.shape, o.dtype) for o in outs),
        in_specs=[vmem] * 6,
        out_specs=(hbm,) * 6,
        scratch_shapes=[pltpu.SemaphoreType.DMA((6,))],
        compiler_params=pltpu.CompilerParams(vmem_limit_bytes=1 << 20),
        name="put_out",
    )(*outs)
    return (*done[:5], done[5][0])


def solution(mesh):
    chips = mesh.shape["seq"] // 2
    fwd, inv = tables()

    def run(*arrays):
        return body(jnp.asarray(fwd), jnp.asarray(inv), chips, *arrays)

    return jax.shard_map(
        run,
        mesh=mesh,
        in_specs=(
            P("seq", "ch"),
            P("seq", "ch"),
            P("seq", "ch"),
            P("seq", "ch"),
            P(None, None, "ch"),
            P(None, "ch"),
            P("ch"),
        ),
        out_specs=(
            P("seq", "ch"),
            P("seq", "ch"),
            P("seq", "ch"),
            P("seq", "ch"),
            P(None, None, "ch"),
            P("ch"),
        ),
        check_vma=False,
    )
```

```python
import functools

import jax
import jax.numpy as jnp
import ml_dtypes
import numpy as np
from jax import lax
from jax.experimental import pallas as pl
from jax.experimental.pallas import tpu as pltpu
from jax.sharding import PartitionSpec as P

F32, BF16 = jnp.float32, jnp.bfloat16
BLK = 128
ROWS = 16
PAD = 8
LANES = 128


def tables():
    order = np.concatenate([np.arange(0, BLK, 2), np.arange(1, BLK, 2)])
    angle = np.outer(np.pi * (2 * order + 1) / (2 * BLK), np.arange(BLK))
    full = np.concatenate([np.cos(angle), -np.sin(angle)], 0)
    high = full.astype(ml_dtypes.bfloat16).astype(np.float64)
    low = full - high
    fwd = np.concatenate([high, high, low], 1)
    inv = np.concatenate([high.T, high.T, low.T], 1) / BLK
    return fwd.astype(ml_dtypes.bfloat16), inv.astype(ml_dtypes.bfloat16)


def kernel(
    chips,
    q_hbm, k_hbm, v_hbm, y_hbm, sf_hbm, lf_hbm, sg_hbm, fwd_hbm, inv_hbm,
    oq, ok, ov, ofilt, otaps, ogain,
    qb, kb, vb, yb, hq, hk, hv, nq, ny, sf, lf, sg, fwd, inv,
    rq, rk, rv, rn, kf, vf, gq, gk, gv, xz, xg, xh, zs, gs, hs, xs, xu, gl_f, xgl,
    mine3, nx, glt, gl_in, racc, rs_in, taps, half, half_in, near, far, fin,
    in_sem, send, recv, known,
):
    length = q_hbm.shape[0]
    width = q_hbm.shape[1]
    tiles = width // LANES
    nblk = length // BLK
    last = nblk - 1
    me = lax.axis_index("seq")
    total = 2 * chips
    z, c = me // 2, lax.rem(me, 2)
    has_prev, has_next = me > 0, me < total - 1
    prev, nxt = me - 1, me + 1
    partner = me + 1 - 2 * c

    def at_chip(chip):
        return lax.rem(chip + chips, chips) * 2 + c

    def remote(src, dst, slot, device):
        return pltpu.make_async_remote_copy(
            src_ref=src, dst_ref=dst, send_sem=send.at[slot], recv_sem=recv.at[slot],
            device_id={"seq": device}, device_id_type=pl.DeviceIdType.MESH,
        )

    def signal(sem, device):
        pl.semaphore_signal(sem, 1, device_id={"seq": device}, device_id_type=pl.DeviceIdType.MESH)

    barrier = pltpu.get_barrier_semaphore()
    signal(barrier, at_chip(z + 1))
    signal(barrier, at_chip(z - 1))

    @pl.when(has_prev)
    def _():
        signal(barrier, prev)

    @pl.when(has_next)
    def _():
        signal(barrier, nxt)

    def load(array, b):
        hbm, buf = ((q_hbm, qb), (k_hbm, kb), (v_hbm, vb), (y_hbm, yb))[array]
        rows = pl.ds(b * BLK, BLK)
        return pltpu.make_async_copy(hbm.at[rows], buf.at[rows], in_sem.at[array * nblk + b])

    extra = []
    for n, (hbm, buf) in enumerate(((sf_hbm, sf), (lf_hbm, lf), (sg_hbm, sg), (fwd_hbm, fwd), (inv_hbm, inv))):
        extra.append(pltpu.make_async_copy(hbm, buf, in_sem.at[4 * nblk + n]))

    extra[0].start()
    early = [(1, last - 1), (2, last - 1), (1, last), (2, last), (0, 0), (3, 0), (0, last)]
    for key in early:
        load(*key).start()
    for copy in extra[1:4]:
        copy.start()
    for b in range(nblk):
        for array in (1, 2, 0, 3):
            if (array, b) not in early:
                load(array, b).start()
    extra[4].start()
    waited = set()

    def ready(*keys):
        for key in keys:
            if key not in waited:
                waited.add(key)
                load(*key).wait()

    @pl.when(jnp.logical_not(has_prev))
    def _():
        for buf in (hq, hk, hv):
            buf[...] = jnp.zeros_like(buf)
        xz[0, 0 : 2 * BLK, :] = jnp.zeros((2 * BLK, width), BF16)

    @pl.when(jnp.logical_not(has_next))
    def _():
        nq[...] = jnp.zeros_like(nq)
        ny[...] = jnp.zeros_like(ny)
        xg[nblk, 0 : 2 * BLK, :] = jnp.zeros((2 * BLK, width), BF16)
        nx[...] = jnp.zeros_like(nx)

    for h in range(2):
        half[h, 2] = jnp.zeros((8, LANES), F32)

    def by_tile(body):
        for j in range(tiles):
            body(j, slice(j * LANES, (j + 1) * LANES))

    def weights(which, lanes):
        return [sf[which, i : i + 1, lanes] for i in range(3)]

    def widen(buf, raw, j, lanes, r0, r1):
        raw[j, PAD + r0 : PAD + r1, :] = buf[r0:r1, lanes].astype(F32)

    def feat(raw, j, w, r0, r1):
        return (
            w[0] * raw[j, PAD + r0 : PAD + r1, :]
            + w[1] * raw[j, PAD + r0 - 1 : PAD + r1 - 1, :]
            + w[2] * raw[j, PAD + r0 - 2 : PAD + r1 - 2, :]
        )

    def put(ref, b, n, lanes, value):
        size = value.shape[0]
        high = value.astype(BF16)
        low = (value - high.astype(F32)).astype(BF16)
        ref[b, n : n + size, lanes] = high
        ref[b, BLK + n : BLK + n + size, lanes] = low
        ref[b, 2 * BLK + n : 2 * BLK + n + size, lanes] = high

    def z_rows(b, n0, n1, wide=True):
        def body(j, lanes):
            wk, wv = weights(1, lanes), weights(2, lanes)
            if wide:
                widen(kb, rk, j, lanes, b * BLK + n0, b * BLK + n1)
                widen(vb, rv, j, lanes, b * BLK + n0, b * BLK + n1)
            for n in range(n0, n1, ROWS):
                r0 = b * BLK + n
                kk, vv = feat(rk, j, wk, r0, r0 + ROWS), feat(rv, j, wv, r0, r0 + ROWS)
                kf[j, r0 : r0 + ROWS, :] = kk
                vf[j, r0 : r0 + ROWS, :] = vv
                put(xz, b + 1, n, lanes, kk * vv)

        by_tile(body)

    def g_rows(b, n0, n1, wide=True):
        def body(j, lanes):
            wq = weights(0, lanes)
            if wide:
                widen(qb, rq, j, lanes, b * BLK + n0, b * BLK + n1)
            for n in range(n0, n1, ROWS):
                r0 = b * BLK + n
                put(xg, b, n, lanes, yb[r0 : r0 + ROWS, lanes].astype(F32) * feat(rq, j, wq, r0, r0 + ROWS))

        by_tile(body)

    extra[0].wait()
    ready((1, last - 1), (2, last - 1), (1, last), (2, last))

    def before_last(j, lanes):
        widen(kb, rk, j, lanes, last * BLK - ROWS, last * BLK)
        widen(vb, rv, j, lanes, last * BLK - ROWS, last * BLK)

    by_tile(before_last)
    z_rows(last, 0, BLK)
    ready((0, 0), (3, 0))
    by_tile(lambda j, lanes: widen(qb, rq, j, lanes, 0, ROWS))
    g_rows(0, ROWS, BLK)
    ready((0, last))

    count = 2 + has_prev.astype(jnp.int32) + has_next.astype(jnp.int32)
    pl.semaphore_wait(barrier, count)
    tail = pl.ds(length - PAD, PAD)
    to_next = [remote(buf.at[tail], hist, n, nxt) for n, (buf, hist) in enumerate(((qb, hq), (kb, hk), (vb, hv)))]
    z_halo = remote(xz.at[nblk, pl.ds(0, 2 * BLK)], xz.at[0, pl.ds(0, 2 * BLK)], 3, nxt)
    head = pl.ds(0, ROWS)
    to_prev = [remote(qb.at[head], nq, 4, prev), remote(yb.at[head], ny, 5, prev)]
    g_halo = [
        remote(xg.at[0, pl.ds(h * BLK + ROWS, BLK - ROWS)], xg.at[nblk, pl.ds(h * BLK + ROWS, BLK - ROWS)], 6 + h, prev)
        for h in range(2)
    ]

    @pl.when(has_next)
    def _():
        for copy in to_next:
            copy.start()
        z_halo.start()

    @pl.when(has_prev)
    def _():
        for copy in to_prev + g_halo:
            copy.start()

    steps = []
    radius = 1
    while radius < chips // 2:
        steps.append(radius)
        radius *= 2

    def tell(n):
        if n < len(steps):
            signal(known.at[n], at_chip(z + steps[n]))
            signal(known.at[n], at_chip(z - steps[n]))

    def learn(n):
        if n < len(steps):
            pl.semaphore_wait(known.at[n], 2)

    tell(0)

    for b in range(nblk):
        ready((0, b), (1, b), (2, b), (3, b))
    for copy in extra[1:]:
        copy.wait()
    def filter_rows(j, lanes):
        first = lf[0:ROWS, lanes]
        at_zero = lax.broadcasted_iota(jnp.int32, (ROWS, LANES), 0) == 0
        put(xh, 0, 0, lanes, jnp.where(at_zero, first + sg[:, lanes], first))
        put(xh, 0, ROWS, lanes, lf[ROWS:BLK, lanes])

    def dft(x, b, out, o):
        for lane in range(0, width, 256):
            cols = slice(lane, lane + 256)
            out[o, :, cols] = jnp.dot(fwd[...], x[b, :, cols], preferred_element_type=F32)

    by_tile(lambda j, lanes: (widen(kb, rk, j, lanes, 0, ROWS), widen(vb, rv, j, lanes, 0, ROWS)))
    by_tile(filter_rows)
    g_rows(1, 0, BLK)
    dft(xh, 0, hs, 0)
    dft(xz, nblk, zs, nblk)
    z_rows(0, ROWS, BLK)
    dft(xg, 1, gs, 1)
    z_rows(1, 0, BLK)
    g_rows(2, 0, BLK)
    dft(xz, 2, zs, 2)
    learn(0)
    tell(1)
    z_rows(2, 0, BLK)
    dft(xg, 2, gs, 2)
    g_rows(last, 0, BLK)
    dft(xz, last, zs, last)
    dft(xg, last, gs, last)
    @pl.when(has_prev)
    def _():
        for copy in to_next:
            copy.wait_recv()

    def history(j, lanes):
        for raw, hist in ((rq, hq), (rk, hk), (rv, hv)):
            raw[j, 0:PAD, :] = hist[:, lanes].astype(F32)

    by_tile(history)
    z_rows(0, 0, ROWS, False)
    g_rows(0, 0, ROWS, False)
    dft(xz, 1, zs, 1)
    dft(xg, 0, gs, 0)

    def put_spectrum(ref, b, k, lanes, real, imag):
        for off, value in ((0, real), (BLK, imag)):
            high = value.astype(BF16)
            low = (value - high.astype(F32)).astype(BF16)
            ref[b, off + k : off + k + ROWS, lanes] = high
            ref[b, 2 * BLK + off + k : 2 * BLK + off + k + ROWS, lanes] = low
            ref[b, 4 * BLK + off + k : 4 * BLK + off + k + ROWS, lanes] = high

    def add(a, sign, b):
        return a + b if sign > 0 else a - b

    def frequencies():
        for k in range(0, BLK, ROWS):
            yield k, slice(k, k + ROWS), slice(BLK + k, BLK + k + ROWS), 1 if k < BLK // 2 else -1

    def z_stage(blocks, mode):
        def body(j, lanes):
            for k, re, im, sign in frequencies():
                hr, hi = hs[0, re, lanes], hs[0, im, lanes]
                lr = li = None
                if mode != "first":
                    lr, li = gl_f[re, lanes], gl_f[im, lanes]
                for b in blocks:
                    vr = add(zs[b + 1, re, lanes], -sign, zs[b, im, lanes])
                    vi = add(zs[b + 1, im, lanes], sign, zs[b, re, lanes])
                    gr, gi = gs[b, re, lanes], gs[b, im, lanes]
                    pr, pi = gr * vr + gi * vi, gi * vr - gr * vi
                    lr, li = (pr, pi) if lr is None else (lr + pr, li + pi)
                    put_spectrum(xs, b, k, lanes, hr * vr - hi * vi, hr * vi + hi * vr)
                if mode == "last":
                    put_spectrum(xgl, 0, k, lanes, lr, li)
                else:
                    gl_f[re, lanes] = lr
                    gl_f[im, lanes] = li

        by_tile(body)

    def g_stage(blocks):
        def body(j, lanes):
            for k, re, im, sign in frequencies():
                hr, hi = hs[0, re, lanes], hs[0, im, lanes]
                for b in blocks:
                    ur = add(gs[b, re, lanes], sign, gs[b + 1, im, lanes])
                    ui = add(gs[b, im, lanes], -sign, gs[b + 1, re, lanes])
                    put_spectrum(xu, b, k, lanes, hr * ur + hi * ui, hr * ui - hi * ur)

        by_tile(body)

    def inverse(x, b, use):
        for lane in range(0, width, 256):
            value = jnp.dot(inv[...], x[b, :, lane : lane + 256], preferred_element_type=F32)
            for part in range(0, 256, LANES):
                use(b, (lane + part) // LANES, value[:, part : part + LANES])

    def use_s(b, j, value):
        rows = slice(b * BLK, (b + 1) * BLK)
        gq[j, rows, :] = value * yb[rows, LANES * j : LANES * (j + 1)].astype(F32)

    def use_gz(b, j, value):
        rows = slice(b * BLK, (b + 1) * BLK)
        gk[j, rows, :] = value * vf[j, rows, :]
        gv[j, rows, :] = value * kf[j, rows, :]

    kinds = ((gq, rq, oq), (gk, rk, ok), (gv, rv, ov))

    def finish(which, r0, r1, fresh=False, write=True, count=True):
        grad, raw, out = kinds[which]

        def body(j, lanes):
            w = weights(which, lanes)
            sums = [None if fresh else taps[3 * which + i, j] for i in range(3)] if count else None
            for r in range(r0, r1, ROWS):
                own = grad[j, r : r + ROWS, :]
                if write:
                    one, two = grad[j, r + 1 : r + 1 + ROWS, :], grad[j, r + 2 : r + 2 + ROWS, :]
                    out[r : r + ROWS, lanes] = (w[0] * own + w[1] * one + w[2] * two).astype(BF16)
                if count:
                    for i in range(3):
                        product = own * raw[j, PAD + r - i : PAD + r - i + ROWS, :]
                        product = product[0:8] + product[8:16]
                        sums[i] = product if sums[i] is None else sums[i] + product
            if count:
                for i in range(3):
                    taps[3 * which + i, j] = sums[i]

        by_tile(body)

    z_stage((1,), "first")
    learn(1)
    tell(2)
    z_stage((2,), "more")
    inverse(xs, 1, use_s)
    z_stage((3,), "more")
    inverse(xs, 2, use_s)
    g_stage((0,))
    inverse(xs, 3, use_s)
    finish(0, BLK, 3 * BLK - ROWS, True)
    g_stage((1,))
    inverse(xu, 0, use_gz)
    finish(0, 3 * BLK - ROWS, length - ROWS)
    finish(0, length - ROWS, length, write=False)
    g_stage((2,))
    inverse(xu, 1, use_gz)
    finish(1, 0, BLK - ROWS, True)
    finish(2, 0, BLK - ROWS, True)
    inverse(xu, 2, use_gz)
    finish(1, BLK - ROWS, 2 * BLK - ROWS)
    finish(2, BLK - ROWS, 2 * BLK - ROWS)
    finish(1, 2 * BLK - ROWS, 3 * BLK - ROWS)
    finish(2, 2 * BLK - ROWS, 3 * BLK - ROWS)


    @pl.when(has_prev)
    def _():
        z_halo.wait_recv()

    @pl.when(has_next)
    def _():
        for copy in to_prev + g_halo:
            copy.wait_recv()

    share = BLK // total

    def next_rows(j, lanes):
        w = weights(0, lanes)
        rn[j, 0:PAD, :] = rq[j, length : length + PAD, :]
        rn[j, PAD : PAD + ROWS, :] = nq[:, lanes].astype(F32)
        put(xg, nblk, 0, lanes, ny[:, lanes].astype(F32) * feat(rn, j, w, 0, ROWS))

    def use_gl(b, j, value):
        cols = slice(LANES * j, LANES * (j + 1))
        for i in range(total):
            glt[i % 2, i // 2, :, cols] = value[share * i : share * (i + 1), :]
        half[j // 2, 2, 2 * (j % 2) + 1 : 2 * (j % 2) + 2, :] = value[0:1, :]

    xz[0, 2 * BLK :, :] = xz[0, 0:BLK, :]
    by_tile(next_rows)
    xg[nblk, 2 * BLK + ROWS :, :] = xg[nblk, ROWS:BLK, :]
    dft(xz, 0, zs, 0)
    dft(xg, nblk, gs, nblk)
    z_stage((0,), "last")
    g_stage((last,))
    inverse(xs, 0, use_s)
    inverse(xgl, 0, use_gl)
    inverse(xu, last, use_gz)
    row = lax.broadcasted_iota(jnp.int32, (8, LANES), 0)
    for j in range(tiles):
        second, third = pltpu.roll(gk[j, 0:8, :], 2, 0), pltpu.roll(gv[j, 0:8, :], 4, 0)
        mine3[j] = jnp.where(row < 2, gq[j, 0:8, :], jnp.where(row < 4, second, third))
    to_partner = remote(glt.at[1 - c], gl_in, 8, partner)
    to_partner.start()
    finish(0, 0, BLK)
    for which in (1, 2):
        finish(which, last * BLK - ROWS, length - ROWS)
        finish(which, length - ROWS, length, write=False)
    for j in range(tiles):
        h, jj = j // 2, j % 2
        for n in range(9):
            total_n = jnp.sum(taps[n, j], axis=0, keepdims=True)
            if n < 8:
                half[h, jj, n : n + 1, :] = total_n
            else:
                half[h, 2, 2 * jj : 2 * jj + 1, :] = total_n
    halves = remote(half.at[1 - c], half_in, 10, partner)
    halves.start()
    firsts = remote(mine3, nx, 9, prev)

    @pl.when(has_prev)
    def _():
        firsts.start()

    to_partner.wait_recv()
    racc[...] = glt[c] + gl_in[...]
    halves.wait_recv()
    group = min(4, chips)
    base = z // group * group
    place, mine = z - base, z // group
    groups = chips // group
    learn(2)
    far[mine] = half[c] + half_in[...]
    distant = []
    for d in sorted(range(1, groups), key=lambda d: -min(d, groups - d)):
        copy = remote(far.at[mine], far.at[mine], 20 + chips + d, at_chip(z + d * group))
        copy.start()
        distant.append(copy)
    scatter = []
    for d in sorted(range(1, chips), key=lambda d: (-min(d, chips - d), d)):
        chip = lax.rem(z + d, chips)
        copy = remote(racc.at[chip], rs_in.at[d], 16 + d, at_chip(chip))
        copy.start()
        scatter.append(copy)

    @pl.when(has_next)
    def _():
        firsts.wait_recv()

    for j in range(tiles):
        gq[j, length : length + 8, :] = nx[j]
        gk[j, length : length + 8, :] = pltpu.roll(nx[j], 6, 0)
        gv[j, length : length + 8, :] = pltpu.roll(nx[j], 4, 0)
    for which in range(3):
        finish(which, length - ROWS, length, count=False)

    for copy in distant:
        copy.wait_recv()
    summed = far[0]
    for n in range(1, groups):
        summed = summed + far[n]
    near[place] = summed
    close = []
    for d in range(1, group):
        copy = remote(near.at[place], near.at[place], 16 + chips + d, at_chip(base + lax.rem(place + d, group)))
        copy.start()
        close.append(copy)

    for copy in scatter:
        copy.wait_recv()
    mine_taps = racc[z]
    for d in range(1, chips):
        mine_taps = mine_taps + rs_in[d]
    ofilt[...] = mine_taps

    for copy in close:
        copy.wait_recv()
    whole = near[0]
    for n in range(1, group):
        whole = whole + near[n]
    fin[c] = whole
    final = remote(fin.at[c], fin.at[c], 11, partner)
    final.start()
    final.wait_recv()
    for h in range(2):
        for j in range(2):
            cols = slice(256 * h + 128 * j, 256 * h + 128 * (j + 1))
            for i in range(8):
                otaps[i // 3, i % 3 : i % 3 + 1, cols] = fin[h, j, i : i + 1, :]
            otaps[2, 2:3, cols] = fin[h, 2, 2 * j : 2 * j + 1, :]
            ogain[0:1, cols] = fin[h, 2, 2 * j + 1 : 2 * j + 2, :]

    @pl.when(has_next)
    def _():
        for copy in to_next:
            copy.wait_send()
        z_halo.wait_send()

    @pl.when(has_prev)
    def _():
        for copy in to_prev + g_halo + [firsts]:
            copy.wait_send()

    for copy in [to_partner, halves, final] + close + distant + scatter:
        copy.wait_send()


def put_out(*refs):
    sem = refs[-1]
    copies = [pltpu.make_async_copy(refs[n], refs[n + 6], sem.at[n]) for n in range(6)]
    for copy in copies:
        copy.start()
    for copy in copies:
        copy.wait()


def body(fwd, inv, chips, input_q, input_k, input_v, grad_out, short_filters, long_filter, skip_gain):
    length, width = input_q.shape
    nblk = length // BLK
    hbm = pl.BlockSpec(memory_space=pltpu.HBM)
    vmem = pl.BlockSpec(memory_space=pltpu.VMEM)
    tiles = width // LANES
    share = BLK // (2 * chips)
    scratch = [
        *(pltpu.VMEM((length, width), BF16) for _ in range(4)),
        *(pltpu.VMEM((PAD, width), BF16) for _ in range(3)),
        *(pltpu.VMEM((ROWS, width), BF16) for _ in range(2)),
        pltpu.VMEM(short_filters.shape, F32),
        pltpu.VMEM(long_filter.shape, F32),
        pltpu.VMEM((1, width), F32),
        pltpu.VMEM(fwd.shape, BF16),
        pltpu.VMEM(inv.shape, BF16),
        *(pltpu.VMEM((tiles, PAD + length, LANES), F32) for _ in range(3)),
        pltpu.VMEM((tiles, PAD + ROWS, LANES), F32),
        *(pltpu.VMEM((tiles, length, LANES), F32) for _ in range(2)),
        *(pltpu.VMEM((tiles, length + 8, LANES), F32) for _ in range(3)),
        pltpu.VMEM((nblk + 1, 3 * BLK, width), BF16),
        pltpu.VMEM((nblk + 1, 3 * BLK, width), BF16),
        pltpu.VMEM((1, 3 * BLK, width), BF16),
        pltpu.VMEM((nblk + 1, 2 * BLK, width), F32),
        pltpu.VMEM((nblk + 1, 2 * BLK, width), F32),
        pltpu.VMEM((1, 2 * BLK, width), F32),
        pltpu.VMEM((nblk, 6 * BLK, width), BF16),
        pltpu.VMEM((nblk, 6 * BLK, width), BF16),
        pltpu.VMEM((2 * BLK, width), F32),
        pltpu.VMEM((1, 6 * BLK, width), BF16),
        pltpu.VMEM((tiles, 8, LANES), F32),
        pltpu.VMEM((tiles, 8, LANES), F32),
        pltpu.VMEM((2, chips, share, width), F32),
        pltpu.VMEM((chips, share, width), F32),
        pltpu.VMEM((chips, share, width), F32),
        pltpu.VMEM((chips, share, width), F32),
        pltpu.VMEM((9, tiles, 8, LANES), F32),
        pltpu.VMEM((2, 3, 8, LANES), F32),
        pltpu.VMEM((3, 8, LANES), F32),
        pltpu.VMEM((4, 3, 8, LANES), F32),
        pltpu.VMEM((4, 3, 8, LANES), F32),
        pltpu.VMEM((2, 3, 8, LANES), F32),
        pltpu.SemaphoreType.DMA((4 * nblk + 5,)),
        pltpu.SemaphoreType.DMA((32 + chips,)),
        pltpu.SemaphoreType.DMA((32 + chips,)),
        pltpu.SemaphoreType.REGULAR((3,)),
    ]
    operands = (input_q, input_k, input_v, grad_out, short_filters, long_filter, skip_gain[None], fwd, inv)
    outs = pl.pallas_call(
        functools.partial(kernel, chips),
        out_shape=(
            *(pltpu.VMEM((length, width), BF16) for _ in range(3)),
            pltpu.VMEM((BLK // (2 * chips), width), F32),
            pltpu.VMEM(short_filters.shape, F32),
            pltpu.VMEM((1, width), F32),
        ),
        in_specs=[hbm] * 9,
        out_specs=(vmem,) * 6,
        scratch_shapes=scratch,
        compiler_params=pltpu.CompilerParams(
            collective_id=0, has_side_effects=True, vmem_limit_bytes=48 * 1024 * 1024
        ),
        name="hyena_backward",
    )(*(pltpu.with_memory_space_constraint(a, pltpu.HBM) for a in operands))
    done = pl.pallas_call(
        put_out,
        out_shape=tuple(jax.ShapeDtypeStruct(o.shape, o.dtype) for o in outs),
        in_specs=[vmem] * 6,
        out_specs=(hbm,) * 6,
        scratch_shapes=[pltpu.SemaphoreType.DMA((6,))],
        compiler_params=pltpu.CompilerParams(vmem_limit_bytes=1 << 20),
        name="put_out",
    )(*outs)
    return (*done[:5], done[5][0])


def solution(mesh):
    chips = mesh.shape["seq"] // 2
    fwd, inv = tables()

    def run(*arrays):
        return body(jnp.asarray(fwd), jnp.asarray(inv), chips, *arrays)

    return jax.shard_map(
        run,
        mesh=mesh,
        in_specs=(
            P("seq", "ch"),
            P("seq", "ch"),
            P("seq", "ch"),
            P("seq", "ch"),
            P(None, None, "ch"),
            P(None, "ch"),
            P("ch"),
        ),
        out_specs=(
            P("seq", "ch"),
            P("seq", "ch"),
            P("seq", "ch"),
            P("seq", "ch"),
            P(None, None, "ch"),
            P("ch"),
        ),
        check_vma=False,
    )
```

```python
import functools

import jax
import jax.numpy as jnp
import ml_dtypes
import numpy as np
from jax import lax
from jax.experimental import pallas as pl
from jax.experimental.pallas import tpu as pltpu
from jax.sharding import PartitionSpec as P

F32, BF16 = jnp.float32, jnp.bfloat16
BLK = 128
ROWS = 16
PAD = 8
LANES = 128


def tables():
    order = np.concatenate([np.arange(0, BLK, 2), np.arange(1, BLK, 2)])
    angle = np.outer(np.pi * (2 * order + 1) / (2 * BLK), np.arange(BLK))
    full = np.concatenate([np.cos(angle), -np.sin(angle)], 0)
    high = full.astype(ml_dtypes.bfloat16).astype(np.float64)
    low = full - high
    fwd = np.concatenate([high, high, low], 1)
    inv = np.concatenate([high.T, high.T, low.T], 1) / BLK
    return fwd.astype(ml_dtypes.bfloat16), inv.astype(ml_dtypes.bfloat16)


def kernel(
    chips,
    q_hbm, k_hbm, v_hbm, y_hbm, sf_hbm, lf_hbm, sg_hbm, fwd_hbm, inv_hbm,
    oq, ok, ov, ofilt, otaps, ogain,
    qb, kb, vb, yb, hq, hk, hv, nq, ny, sf, lf, sg, fwd, inv,
    rq, rk, rv, rn, kf, vf, gq, gk, gv, xz, xg, xh, zs, gs, hs, xs, xu, gl_f, xgl,
    mine3, nx, glt, gl_in, racc, rs_in, taps, half, half_in, near, far, fin,
    in_sem, send, recv, known,
):
    length = q_hbm.shape[0]
    width = q_hbm.shape[1]
    tiles = width // LANES
    nblk = length // BLK
    last = nblk - 1
    me = lax.axis_index("seq")
    total = 2 * chips
    z, c = me // 2, lax.rem(me, 2)
    has_prev, has_next = me > 0, me < total - 1
    prev, nxt = me - 1, me + 1
    partner = me + 1 - 2 * c

    def at_chip(chip):
        return lax.rem(chip + chips, chips) * 2 + c

    def remote(src, dst, slot, device):
        return pltpu.make_async_remote_copy(
            src_ref=src, dst_ref=dst, send_sem=send.at[slot], recv_sem=recv.at[slot],
            device_id={"seq": device}, device_id_type=pl.DeviceIdType.MESH,
        )

    def signal(sem, device):
        pl.semaphore_signal(sem, 1, device_id={"seq": device}, device_id_type=pl.DeviceIdType.MESH)

    barrier = pltpu.get_barrier_semaphore()
    signal(barrier, at_chip(z + 1))
    signal(barrier, at_chip(z - 1))

    @pl.when(has_prev)
    def _():
        signal(barrier, prev)

    @pl.when(has_next)
    def _():
        signal(barrier, nxt)

    def load(array, b):
        hbm, buf = ((q_hbm, qb), (k_hbm, kb), (v_hbm, vb), (y_hbm, yb))[array]
        rows = pl.ds(b * BLK, BLK)
        return pltpu.make_async_copy(hbm.at[rows], buf.at[rows], in_sem.at[array * nblk + b])

    extra = []
    for n, (hbm, buf) in enumerate(((sf_hbm, sf), (lf_hbm, lf), (sg_hbm, sg), (fwd_hbm, fwd), (inv_hbm, inv))):
        extra.append(pltpu.make_async_copy(hbm, buf, in_sem.at[4 * nblk + n]))

    extra[0].start()
    early = [(1, last - 1), (2, last - 1), (1, last), (2, last), (0, 0), (3, 0), (0, last)]
    for key in early:
        load(*key).start()
    for copy in extra[1:4]:
        copy.start()
    for b in range(nblk):
        for array in (1, 2, 0, 3):
            if (array, b) not in early:
                load(array, b).start()
    extra[4].start()
    waited = set()

    def ready(*keys):
        for key in keys:
            if key not in waited:
                waited.add(key)
                load(*key).wait()

    @pl.when(jnp.logical_not(has_prev))
    def _():
        for buf in (hq, hk, hv):
            buf[...] = jnp.zeros_like(buf)
        xz[0, 0 : 2 * BLK, :] = jnp.zeros((2 * BLK, width), BF16)

    @pl.when(jnp.logical_not(has_next))
    def _():
        nq[...] = jnp.zeros_like(nq)
        ny[...] = jnp.zeros_like(ny)
        xg[nblk, 0 : 2 * BLK, :] = jnp.zeros((2 * BLK, width), BF16)
        nx[...] = jnp.zeros_like(nx)

    for h in range(2):
        half[h, 2] = jnp.zeros((8, LANES), F32)

    def by_tile(body):
        for j in range(tiles):
            body(j, slice(j * LANES, (j + 1) * LANES))

    def weights(which, lanes):
        return [sf[which, i : i + 1, lanes] for i in range(3)]

    def widen(buf, raw, j, lanes, r0, r1):
        raw[j, PAD + r0 : PAD + r1, :] = buf[r0:r1, lanes].astype(F32)

    def feat(raw, j, w, r0, r1):
        return (
            w[0] * raw[j, PAD + r0 : PAD + r1, :]
            + w[1] * raw[j, PAD + r0 - 1 : PAD + r1 - 1, :]
            + w[2] * raw[j, PAD + r0 - 2 : PAD + r1 - 2, :]
        )

    def put(ref, b, n, lanes, value):
        size = value.shape[0]
        high = value.astype(BF16)
        low = (value - high.astype(F32)).astype(BF16)
        ref[b, n : n + size, lanes] = high
        ref[b, BLK + n : BLK + n + size, lanes] = low
        ref[b, 2 * BLK + n : 2 * BLK + n + size, lanes] = high

    def z_rows(b, n0, n1, wide=True):
        def body(j, lanes):
            wk, wv = weights(1, lanes), weights(2, lanes)
            if wide:
                widen(kb, rk, j, lanes, b * BLK + n0, b * BLK + n1)
                widen(vb, rv, j, lanes, b * BLK + n0, b * BLK + n1)
            for n in range(n0, n1, ROWS):
                r0 = b * BLK + n
                kk, vv = feat(rk, j, wk, r0, r0 + ROWS), feat(rv, j, wv, r0, r0 + ROWS)
                kf[j, r0 : r0 + ROWS, :] = kk
                vf[j, r0 : r0 + ROWS, :] = vv
                put(xz, b + 1, n, lanes, kk * vv)

        by_tile(body)

    def g_rows(b, n0, n1, wide=True):
        def body(j, lanes):
            wq = weights(0, lanes)
            if wide:
                widen(qb, rq, j, lanes, b * BLK + n0, b * BLK + n1)
            for n in range(n0, n1, ROWS):
                r0 = b * BLK + n
                put(xg, b, n, lanes, yb[r0 : r0 + ROWS, lanes].astype(F32) * feat(rq, j, wq, r0, r0 + ROWS))

        by_tile(body)

    extra[0].wait()
    ready((1, last - 1), (2, last - 1), (1, last), (2, last))

    def before_last(j, lanes):
        widen(kb, rk, j, lanes, last * BLK - ROWS, last * BLK)
        widen(vb, rv, j, lanes, last * BLK - ROWS, last * BLK)

    by_tile(before_last)
    z_rows(last, 0, BLK)
    ready((0, 0), (3, 0))
    by_tile(lambda j, lanes: widen(qb, rq, j, lanes, 0, ROWS))
    g_rows(0, ROWS, BLK)
    ready((0, last))

    count = 2 + has_prev.astype(jnp.int32) + has_next.astype(jnp.int32)
    pl.semaphore_wait(barrier, count)
    tail = pl.ds(length - PAD, PAD)
    to_next = [remote(buf.at[tail], hist, n, nxt) for n, (buf, hist) in enumerate(((qb, hq), (kb, hk), (vb, hv)))]
    z_halo = remote(xz.at[nblk, pl.ds(0, 2 * BLK)], xz.at[0, pl.ds(0, 2 * BLK)], 3, nxt)
    head = pl.ds(0, ROWS)
    to_prev = [remote(qb.at[head], nq, 4, prev), remote(yb.at[head], ny, 5, prev)]
    g_halo = [
        remote(xg.at[0, pl.ds(h * BLK + ROWS, BLK - ROWS)], xg.at[nblk, pl.ds(h * BLK + ROWS, BLK - ROWS)], 6 + h, prev)
        for h in range(2)
    ]

    @pl.when(has_next)
    def _():
        for copy in to_next:
            copy.start()
        z_halo.start()

    @pl.when(has_prev)
    def _():
        for copy in to_prev + g_halo:
            copy.start()

    steps = []
    radius = 1
    while radius < chips // 2:
        steps.append(radius)
        radius *= 2

    def tell(n):
        if n < len(steps):
            signal(known.at[n], at_chip(z + steps[n]))
            signal(known.at[n], at_chip(z - steps[n]))

    def learn(n):
        if n < len(steps):
            pl.semaphore_wait(known.at[n], 2)

    tell(0)

    for b in range(nblk):
        ready((0, b), (1, b), (2, b), (3, b))
    for copy in extra[1:]:
        copy.wait()
    def filter_rows(j, lanes):
        first = lf[0:ROWS, lanes]
        at_zero = lax.broadcasted_iota(jnp.int32, (ROWS, LANES), 0) == 0
        put(xh, 0, 0, lanes, jnp.where(at_zero, first + sg[:, lanes], first))
        put(xh, 0, ROWS, lanes, lf[ROWS:BLK, lanes])

    def dft(x, b, out, o):
        for lane in range(0, width, 256):
            cols = slice(lane, lane + 256)
            out[o, :, cols] = jnp.dot(fwd[...], x[b, :, cols], preferred_element_type=F32)

    by_tile(lambda j, lanes: (widen(kb, rk, j, lanes, 0, ROWS), widen(vb, rv, j, lanes, 0, ROWS)))
    by_tile(filter_rows)
    g_rows(1, 0, BLK)
    dft(xh, 0, hs, 0)
    dft(xz, nblk, zs, nblk)
    z_rows(0, ROWS, BLK)
    dft(xg, 1, gs, 1)
    z_rows(1, 0, BLK)
    g_rows(2, 0, BLK)
    dft(xz, 2, zs, 2)
    learn(0)
    tell(1)
    z_rows(2, 0, BLK)
    dft(xg, 2, gs, 2)
    g_rows(last, 0, BLK)
    dft(xz, last, zs, last)
    dft(xg, last, gs, last)
    @pl.when(has_prev)
    def _():
        for copy in to_next:
            copy.wait_recv()

    def history(j, lanes):
        for raw, hist in ((rq, hq), (rk, hk), (rv, hv)):
            raw[j, 0:PAD, :] = hist[:, lanes].astype(F32)

    by_tile(history)
    z_rows(0, 0, ROWS, False)
    g_rows(0, 0, ROWS, False)
    dft(xz, 1, zs, 1)
    dft(xg, 0, gs, 0)

    def put_spectrum(ref, b, k, lanes, real, imag):
        for off, value in ((0, real), (BLK, imag)):
            high = value.astype(BF16)
            low = (value - high.astype(F32)).astype(BF16)
            ref[b, off + k : off + k + ROWS, lanes] = high
            ref[b, 2 * BLK + off + k : 2 * BLK + off + k + ROWS, lanes] = low
            ref[b, 4 * BLK + off + k : 4 * BLK + off + k + ROWS, lanes] = high

    def add(a, sign, b):
        return a + b if sign > 0 else a - b

    def frequencies():
        for k in range(0, BLK, ROWS):
            yield k, slice(k, k + ROWS), slice(BLK + k, BLK + k + ROWS), 1 if k < BLK // 2 else -1

    def z_stage(blocks, mode):
        def body(j, lanes):
            for k, re, im, sign in frequencies():
                hr, hi = hs[0, re, lanes], hs[0, im, lanes]
                lr = li = None
                if mode != "first":
                    lr, li = gl_f[re, lanes], gl_f[im, lanes]
                for b in blocks:
                    vr = add(zs[b + 1, re, lanes], -sign, zs[b, im, lanes])
                    vi = add(zs[b + 1, im, lanes], sign, zs[b, re, lanes])
                    gr, gi = gs[b, re, lanes], gs[b, im, lanes]
                    pr, pi = gr * vr + gi * vi, gi * vr - gr * vi
                    lr, li = (pr, pi) if lr is None else (lr + pr, li + pi)
                    put_spectrum(xs, b, k, lanes, hr * vr - hi * vi, hr * vi + hi * vr)
                if mode == "last":
                    put_spectrum(xgl, 0, k, lanes, lr, li)
                else:
                    gl_f[re, lanes] = lr
                    gl_f[im, lanes] = li

        by_tile(body)

    def g_stage(blocks):
        def body(j, lanes):
            for k, re, im, sign in frequencies():
                hr, hi = hs[0, re, lanes], hs[0, im, lanes]
                for b in blocks:
                    ur = add(gs[b, re, lanes], sign, gs[b + 1, im, lanes])
                    ui = add(gs[b, im, lanes], -sign, gs[b + 1, re, lanes])
                    put_spectrum(xu, b, k, lanes, hr * ur + hi * ui, hr * ui - hi * ur)

        by_tile(body)

    def inverse(x, b, use):
        for lane in range(0, width, 256):
            value = jnp.dot(inv[...], x[b, :, lane : lane + 256], preferred_element_type=F32)
            for part in range(0, 256, LANES):
                use(b, (lane + part) // LANES, value[:, part : part + LANES])

    def use_s(b, j, value):
        rows = slice(b * BLK, (b + 1) * BLK)
        gq[j, rows, :] = value * yb[rows, LANES * j : LANES * (j + 1)].astype(F32)

    def use_gz(b, j, value):
        rows = slice(b * BLK, (b + 1) * BLK)
        gk[j, rows, :] = value * vf[j, rows, :]
        gv[j, rows, :] = value * kf[j, rows, :]

    kinds = ((gq, rq, oq), (gk, rk, ok), (gv, rv, ov))

    def finish(which, r0, r1, fresh=False, write=True, count=True):
        grad, raw, out = kinds[which]

        def body(j, lanes):
            w = weights(which, lanes)
            sums = [None if fresh else taps[3 * which + i, j] for i in range(3)] if count else None
            for r in range(r0, r1, ROWS):
                own = grad[j, r : r + ROWS, :]
                if write:
                    one, two = grad[j, r + 1 : r + 1 + ROWS, :], grad[j, r + 2 : r + 2 + ROWS, :]
                    out[r : r + ROWS, lanes] = (w[0] * own + w[1] * one + w[2] * two).astype(BF16)
                if count:
                    for i in range(3):
                        product = own * raw[j, PAD + r - i : PAD + r - i + ROWS, :]
                        product = product[0:8] + product[8:16]
                        sums[i] = product if sums[i] is None else sums[i] + product
            if count:
                for i in range(3):
                    taps[3 * which + i, j] = sums[i]

        by_tile(body)

    z_stage((1,), "first")
    z_stage((2,), "more")
    z_stage((3,), "more")
    learn(1)
    tell(2)

    @pl.when(has_prev)
    def _():
        z_halo.wait_recv()

    share = BLK // total

    def use_gl(b, j, value):
        cols = slice(LANES * j, LANES * (j + 1))
        for i in range(total):
            glt[i % 2, i // 2, :, cols] = value[share * i : share * (i + 1), :]
        half[j // 2, 2, 2 * (j % 2) + 1 : 2 * (j % 2) + 2, :] = value[0:1, :]

    xz[0, 2 * BLK :, :] = xz[0, 0:BLK, :]
    dft(xz, 0, zs, 0)
    z_stage((0,), "last")
    inverse(xgl, 0, use_gl)
    to_partner = remote(glt.at[1 - c], gl_in, 8, partner)
    to_partner.start()
    inverse(xs, 0, use_s)
    g_stage((0,))
    inverse(xu, 0, use_gz)
    g_stage((1,))
    row = lax.broadcasted_iota(jnp.int32, (8, LANES), 0)
    for j in range(tiles):
        second, third = pltpu.roll(gk[j, 0:8, :], 2, 0), pltpu.roll(gv[j, 0:8, :], 4, 0)
        mine3[j] = jnp.where(row < 2, gq[j, 0:8, :], jnp.where(row < 4, second, third))
    firsts = remote(mine3, nx, 9, prev)

    @pl.when(has_prev)
    def _():
        firsts.start()

    inverse(xs, 1, use_s)
    inverse(xu, 1, use_gz)
    finish(0, 0, BLK - ROWS, True)
    finish(1, 0, BLK - ROWS, True)
    finish(2, 0, BLK - ROWS, True)
    to_partner.wait_recv()
    racc[...] = glt[c] + gl_in[...]
    learn(2)
    order = sorted(range(1, chips), key=lambda d: (-min(d, chips - d), d))
    cut = 4 if chips == 16 else 1
    scatter = []

    def send_taps(distances):
        for d in distances:
            chip = lax.rem(z + d, chips)
            copy = remote(racc.at[chip], rs_in.at[d], 16 + d, at_chip(chip))
            copy.start()
            scatter.append(copy)

    send_taps(order[:cut])

    @pl.when(has_next)
    def _():
        for copy in to_prev + g_halo:
            copy.wait_recv()

    def next_rows(j, lanes):
        w = weights(0, lanes)
        rn[j, 0:PAD, :] = rq[j, length : length + PAD, :]
        rn[j, PAD : PAD + ROWS, :] = nq[:, lanes].astype(F32)
        put(xg, nblk, 0, lanes, ny[:, lanes].astype(F32) * feat(rn, j, w, 0, ROWS))

    by_tile(next_rows)
    xg[nblk, 2 * BLK + ROWS :, :] = xg[nblk, ROWS:BLK, :]
    g_stage((2,))
    dft(xg, nblk, gs, nblk)
    inverse(xs, 2, use_s)
    inverse(xu, 2, use_gz)
    finish(0, BLK - ROWS, 2 * BLK - ROWS)
    inverse(xs, 3, use_s)
    g_stage((last,))
    finish(1, BLK - ROWS, 2 * BLK - ROWS)
    finish(2, BLK - ROWS, 2 * BLK - ROWS)
    inverse(xu, last, use_gz)
    finish(0, 2 * BLK - ROWS, length - ROWS)
    finish(0, length - ROWS, length, write=False)
    for which in (1, 2):
        finish(which, 2 * BLK - ROWS, length - ROWS)
        finish(which, length - ROWS, length, write=False)
    for j in range(tiles):
        h, jj = j // 2, j % 2
        for n in range(9):
            total_n = jnp.sum(taps[n, j], axis=0, keepdims=True)
            if n < 8:
                half[h, jj, n : n + 1, :] = total_n
            else:
                half[h, 2, 2 * jj : 2 * jj + 1, :] = total_n
    halves = remote(half.at[1 - c], half_in, 10, partner)
    halves.start()
    halves.wait_recv()
    group = min(4, chips)
    base = z // group * group
    place, mine = z - base, z // group
    groups = chips // group
    far[mine] = half[c] + half_in[...]
    distant = []
    for d in sorted(range(1, groups), key=lambda d: -min(d, groups - d)):
        copy = remote(far.at[mine], far.at[mine], 20 + chips + d, at_chip(z + d * group))
        copy.start()
        distant.append(copy)
    send_taps(order[cut:])

    @pl.when(has_next)
    def _():
        firsts.wait_recv()

    for j in range(tiles):
        gq[j, length : length + 8, :] = nx[j]
        gk[j, length : length + 8, :] = pltpu.roll(nx[j], 6, 0)
        gv[j, length : length + 8, :] = pltpu.roll(nx[j], 4, 0)
    for which in range(3):
        finish(which, length - ROWS, length, count=False)

    for copy in distant:
        copy.wait_recv()
    summed = far[0]
    for n in range(1, groups):
        summed = summed + far[n]
    near[place] = summed
    close = []
    for d in range(1, group):
        copy = remote(near.at[place], near.at[place], 16 + chips + d, at_chip(base + lax.rem(place + d, group)))
        copy.start()
        close.append(copy)

    for copy in scatter:
        copy.wait_recv()
    mine_taps = racc[z]
    for d in range(1, chips):
        mine_taps = mine_taps + rs_in[d]
    ofilt[...] = mine_taps

    for copy in close:
        copy.wait_recv()
    whole = near[0]
    for n in range(1, group):
        whole = whole + near[n]
    fin[c] = whole
    final = remote(fin.at[c], fin.at[c], 11, partner)
    final.start()
    final.wait_recv()
    for h in range(2):
        for j in range(2):
            cols = slice(256 * h + 128 * j, 256 * h + 128 * (j + 1))
            for i in range(8):
                otaps[i // 3, i % 3 : i % 3 + 1, cols] = fin[h, j, i : i + 1, :]
            otaps[2, 2:3, cols] = fin[h, 2, 2 * j : 2 * j + 1, :]
            ogain[0:1, cols] = fin[h, 2, 2 * j + 1 : 2 * j + 2, :]

    @pl.when(has_next)
    def _():
        for copy in to_next:
            copy.wait_send()
        z_halo.wait_send()

    @pl.when(has_prev)
    def _():
        for copy in to_prev + g_halo + [firsts]:
            copy.wait_send()

    for copy in [to_partner, halves, final] + close + distant + scatter:
        copy.wait_send()


def put_out(*refs):
    sem = refs[-1]
    copies = [pltpu.make_async_copy(refs[n], refs[n + 6], sem.at[n]) for n in range(6)]
    for copy in copies:
        copy.start()
    for copy in copies:
        copy.wait()


def body(fwd, inv, chips, input_q, input_k, input_v, grad_out, short_filters, long_filter, skip_gain):
    length, width = input_q.shape
    nblk = length // BLK
    hbm = pl.BlockSpec(memory_space=pltpu.HBM)
    vmem = pl.BlockSpec(memory_space=pltpu.VMEM)
    tiles = width // LANES
    share = BLK // (2 * chips)
    scratch = [
        *(pltpu.VMEM((length, width), BF16) for _ in range(4)),
        *(pltpu.VMEM((PAD, width), BF16) for _ in range(3)),
        *(pltpu.VMEM((ROWS, width), BF16) for _ in range(2)),
        pltpu.VMEM(short_filters.shape, F32),
        pltpu.VMEM(long_filter.shape, F32),
        pltpu.VMEM((1, width), F32),
        pltpu.VMEM(fwd.shape, BF16),
        pltpu.VMEM(inv.shape, BF16),
        *(pltpu.VMEM((tiles, PAD + length, LANES), F32) for _ in range(3)),
        pltpu.VMEM((tiles, PAD + ROWS, LANES), F32),
        *(pltpu.VMEM((tiles, length, LANES), F32) for _ in range(2)),
        *(pltpu.VMEM((tiles, length + 8, LANES), F32) for _ in range(3)),
        pltpu.VMEM((nblk + 1, 3 * BLK, width), BF16),
        pltpu.VMEM((nblk + 1, 3 * BLK, width), BF16),
        pltpu.VMEM((1, 3 * BLK, width), BF16),
        pltpu.VMEM((nblk + 1, 2 * BLK, width), F32),
        pltpu.VMEM((nblk + 1, 2 * BLK, width), F32),
        pltpu.VMEM((1, 2 * BLK, width), F32),
        pltpu.VMEM((nblk, 6 * BLK, width), BF16),
        pltpu.VMEM((nblk, 6 * BLK, width), BF16),
        pltpu.VMEM((2 * BLK, width), F32),
        pltpu.VMEM((1, 6 * BLK, width), BF16),
        pltpu.VMEM((tiles, 8, LANES), F32),
        pltpu.VMEM((tiles, 8, LANES), F32),
        pltpu.VMEM((2, chips, share, width), F32),
        pltpu.VMEM((chips, share, width), F32),
        pltpu.VMEM((chips, share, width), F32),
        pltpu.VMEM((chips, share, width), F32),
        pltpu.VMEM((9, tiles, 8, LANES), F32),
        pltpu.VMEM((2, 3, 8, LANES), F32),
        pltpu.VMEM((3, 8, LANES), F32),
        pltpu.VMEM((4, 3, 8, LANES), F32),
        pltpu.VMEM((4, 3, 8, LANES), F32),
        pltpu.VMEM((2, 3, 8, LANES), F32),
        pltpu.SemaphoreType.DMA((4 * nblk + 5,)),
        pltpu.SemaphoreType.DMA((32 + chips,)),
        pltpu.SemaphoreType.DMA((32 + chips,)),
        pltpu.SemaphoreType.REGULAR((3,)),
    ]
    operands = (input_q, input_k, input_v, grad_out, short_filters, long_filter, skip_gain[None], fwd, inv)
    outs = pl.pallas_call(
        functools.partial(kernel, chips),
        out_shape=(
            *(pltpu.VMEM((length, width), BF16) for _ in range(3)),
            pltpu.VMEM((BLK // (2 * chips), width), F32),
            pltpu.VMEM(short_filters.shape, F32),
            pltpu.VMEM((1, width), F32),
        ),
        in_specs=[hbm] * 9,
        out_specs=(vmem,) * 6,
        scratch_shapes=scratch,
        compiler_params=pltpu.CompilerParams(
            collective_id=0, has_side_effects=True, vmem_limit_bytes=48 * 1024 * 1024
        ),
        name="hyena_backward",
    )(*(pltpu.with_memory_space_constraint(a, pltpu.HBM) for a in operands))
    done = pl.pallas_call(
        put_out,
        out_shape=tuple(jax.ShapeDtypeStruct(o.shape, o.dtype) for o in outs),
        in_specs=[vmem] * 6,
        out_specs=(hbm,) * 6,
        scratch_shapes=[pltpu.SemaphoreType.DMA((6,))],
        compiler_params=pltpu.CompilerParams(vmem_limit_bytes=1 << 20),
        name="put_out",
    )(*outs)
    return (*done[:5], done[5][0])


def solution(mesh):
    chips = mesh.shape["seq"] // 2
    fwd, inv = tables()

    def run(*arrays):
        return body(jnp.asarray(fwd), jnp.asarray(inv), chips, *arrays)

    return jax.shard_map(
        run,
        mesh=mesh,
        in_specs=(
            P("seq", "ch"),
            P("seq", "ch"),
            P("seq", "ch"),
            P("seq", "ch"),
            P(None, None, "ch"),
            P(None, "ch"),
            P("ch"),
        ),
        out_specs=(
            P("seq", "ch"),
            P("seq", "ch"),
            P("seq", "ch"),
            P("seq", "ch"),
            P(None, None, "ch"),
            P("ch"),
        ),
        check_vma=False,
    )
```

```python
import functools

import jax
import jax.numpy as jnp
import ml_dtypes
import numpy as np
from jax import lax
from jax.experimental import pallas as pl
from jax.experimental.pallas import tpu as pltpu
from jax.sharding import PartitionSpec as P

F32, BF16 = jnp.float32, jnp.bfloat16
BLK = 128
ROWS = 16
PAD = 8
LANES = 128


def tables():
    order = np.concatenate([np.arange(0, BLK, 2), np.arange(1, BLK, 2)])
    angle = np.outer(np.pi * (2 * order + 1) / (2 * BLK), np.arange(BLK))
    full = np.concatenate([np.cos(angle), -np.sin(angle)], 0)
    high = full.astype(ml_dtypes.bfloat16).astype(np.float64)
    low = full - high
    fwd = np.concatenate([high, high, low], 1)
    inv = np.concatenate([high.T, high.T, low.T], 1) / BLK
    return fwd.astype(ml_dtypes.bfloat16), inv.astype(ml_dtypes.bfloat16)


def kernel(
    chips,
    q_hbm, k_hbm, v_hbm, y_hbm, sf_hbm, lf_hbm, sg_hbm, fwd_hbm, inv_hbm,
    oq, ok, ov, ofilt, otaps, ogain,
    qb, kb, vb, yb, hq, hk, hv, nq, ny, sf, lf, sg, fwd, inv,
    rq, rk, rv, rn, kf, vf, gq, gk, gv, xz, xg, xh, zs, gs, hs, xs, xu, gl_f, xgl,
    mine3, nx, glt, gl_in, racc, rs_in, taps, half, half_in, near, far, fin,
    in_sem, send, recv, known,
):
    length = q_hbm.shape[0]
    width = q_hbm.shape[1]
    tiles = width // LANES
    nblk = length // BLK
    last = nblk - 1
    me = lax.axis_index("seq")
    total = 2 * chips
    z, c = me // 2, lax.rem(me, 2)
    has_prev, has_next = me > 0, me < total - 1
    prev, nxt = me - 1, me + 1
    partner = me + 1 - 2 * c

    def at_chip(chip):
        return lax.rem(chip + chips, chips) * 2 + c

    def remote(src, dst, slot, device):
        return pltpu.make_async_remote_copy(
            src_ref=src, dst_ref=dst, send_sem=send.at[slot], recv_sem=recv.at[slot],
            device_id={"seq": device}, device_id_type=pl.DeviceIdType.MESH,
        )

    def signal(sem, device):
        pl.semaphore_signal(sem, 1, device_id={"seq": device}, device_id_type=pl.DeviceIdType.MESH)

    barrier = pltpu.get_barrier_semaphore()
    signal(barrier, at_chip(z + 1))
    signal(barrier, at_chip(z - 1))

    @pl.when(has_prev)
    def _():
        signal(barrier, prev)

    @pl.when(has_next)
    def _():
        signal(barrier, nxt)

    def load(array, b):
        hbm, buf = ((q_hbm, qb), (k_hbm, kb), (v_hbm, vb), (y_hbm, yb))[array]
        rows = pl.ds(b * BLK, BLK)
        return pltpu.make_async_copy(hbm.at[rows], buf.at[rows], in_sem.at[array * nblk + b])

    extra = []
    for n, (hbm, buf) in enumerate(((sf_hbm, sf), (lf_hbm, lf), (sg_hbm, sg), (fwd_hbm, fwd), (inv_hbm, inv))):
        extra.append(pltpu.make_async_copy(hbm, buf, in_sem.at[4 * nblk + n]))

    extra[0].start()
    early = [(1, last - 1), (2, last - 1), (1, last), (2, last), (0, 0), (3, 0), (0, last)]
    for key in early:
        load(*key).start()
    for copy in extra[1:4]:
        copy.start()
    for b in range(nblk):
        for array in (1, 2, 0, 3):
            if (array, b) not in early:
                load(array, b).start()
    extra[4].start()
    waited = set()

    def ready(*keys):
        for key in keys:
            if key not in waited:
                waited.add(key)
                load(*key).wait()

    @pl.when(jnp.logical_not(has_prev))
    def _():
        for buf in (hq, hk, hv):
            buf[...] = jnp.zeros_like(buf)
        xz[0, 0 : 2 * BLK, :] = jnp.zeros((2 * BLK, width), BF16)

    @pl.when(jnp.logical_not(has_next))
    def _():
        nq[...] = jnp.zeros_like(nq)
        ny[...] = jnp.zeros_like(ny)
        xg[nblk, 0 : 2 * BLK, :] = jnp.zeros((2 * BLK, width), BF16)
        nx[...] = jnp.zeros_like(nx)

    for h in range(2):
        half[h, 2] = jnp.zeros((8, LANES), F32)

    def by_tile(body):
        for j in range(tiles):
            body(j, slice(j * LANES, (j + 1) * LANES))

    def weights(which, lanes):
        return [sf[which, i : i + 1, lanes] for i in range(3)]

    def widen(buf, raw, j, lanes, r0, r1):
        raw[j, PAD + r0 : PAD + r1, :] = buf[r0:r1, lanes].astype(F32)

    def feat(raw, j, w, r0, r1):
        return (
            w[0] * raw[j, PAD + r0 : PAD + r1, :]
            + w[1] * raw[j, PAD + r0 - 1 : PAD + r1 - 1, :]
            + w[2] * raw[j, PAD + r0 - 2 : PAD + r1 - 2, :]
        )

    def put(ref, b, n, lanes, value):
        size = value.shape[0]
        high = value.astype(BF16)
        low = (value - high.astype(F32)).astype(BF16)
        ref[b, n : n + size, lanes] = high
        ref[b, BLK + n : BLK + n + size, lanes] = low
        ref[b, 2 * BLK + n : 2 * BLK + n + size, lanes] = high

    def z_rows(b, n0, n1, wide=True):
        def body(j, lanes):
            wk, wv = weights(1, lanes), weights(2, lanes)
            if wide:
                widen(kb, rk, j, lanes, b * BLK + n0, b * BLK + n1)
                widen(vb, rv, j, lanes, b * BLK + n0, b * BLK + n1)
            for n in range(n0, n1, ROWS):
                r0 = b * BLK + n
                kk, vv = feat(rk, j, wk, r0, r0 + ROWS), feat(rv, j, wv, r0, r0 + ROWS)
                kf[j, r0 : r0 + ROWS, :] = kk
                vf[j, r0 : r0 + ROWS, :] = vv
                put(xz, b + 1, n, lanes, kk * vv)

        by_tile(body)

    def g_rows(b, n0, n1, wide=True):
        def body(j, lanes):
            wq = weights(0, lanes)
            if wide:
                widen(qb, rq, j, lanes, b * BLK + n0, b * BLK + n1)
            for n in range(n0, n1, ROWS):
                r0 = b * BLK + n
                put(xg, b, n, lanes, yb[r0 : r0 + ROWS, lanes].astype(F32) * feat(rq, j, wq, r0, r0 + ROWS))

        by_tile(body)

    extra[0].wait()
    ready((1, last - 1), (2, last - 1), (1, last), (2, last))

    def before_last(j, lanes):
        widen(kb, rk, j, lanes, last * BLK - ROWS, last * BLK)
        widen(vb, rv, j, lanes, last * BLK - ROWS, last * BLK)

    by_tile(before_last)
    z_rows(last, 0, BLK)
    ready((0, 0), (3, 0))
    by_tile(lambda j, lanes: widen(qb, rq, j, lanes, 0, ROWS))
    g_rows(0, ROWS, BLK)
    ready((0, last))

    count = 2 + has_prev.astype(jnp.int32) + has_next.astype(jnp.int32)
    pl.semaphore_wait(barrier, count)
    tail = pl.ds(length - PAD, PAD)
    to_next = [remote(buf.at[tail], hist, n, nxt) for n, (buf, hist) in enumerate(((qb, hq), (kb, hk), (vb, hv)))]
    z_halo = remote(xz.at[nblk, pl.ds(0, 2 * BLK)], xz.at[0, pl.ds(0, 2 * BLK)], 3, nxt)
    head = pl.ds(0, ROWS)
    to_prev = [remote(qb.at[head], nq, 4, prev), remote(yb.at[head], ny, 5, prev)]
    g_halo = [
        remote(xg.at[0, pl.ds(h * BLK + ROWS, BLK - ROWS)], xg.at[nblk, pl.ds(h * BLK + ROWS, BLK - ROWS)], 6 + h, prev)
        for h in range(2)
    ]

    @pl.when(has_next)
    def _():
        for copy in to_next:
            copy.start()
        z_halo.start()

    @pl.when(has_prev)
    def _():
        for copy in to_prev + g_halo:
            copy.start()

    steps = []
    radius = 1
    while radius < chips // 2:
        steps.append(radius)
        radius *= 2

    def tell(n):
        if n < len(steps):
            signal(known.at[n], at_chip(z + steps[n]))
            signal(known.at[n], at_chip(z - steps[n]))

    def learn(n):
        if n < len(steps):
            pl.semaphore_wait(known.at[n], 2)

    tell(0)

    for b in range(nblk):
        ready((0, b), (1, b), (2, b), (3, b))
    for copy in extra[1:]:
        copy.wait()
    def filter_rows(j, lanes):
        first = lf[0:ROWS, lanes]
        at_zero = lax.broadcasted_iota(jnp.int32, (ROWS, LANES), 0) == 0
        put(xh, 0, 0, lanes, jnp.where(at_zero, first + sg[:, lanes], first))
        put(xh, 0, ROWS, lanes, lf[ROWS:BLK, lanes])

    def dft(x, b, out, o):
        for lane in range(0, width, 256):
            cols = slice(lane, lane + 256)
            out[o, :, cols] = jnp.dot(fwd[...], x[b, :, cols], preferred_element_type=F32)

    by_tile(lambda j, lanes: (widen(kb, rk, j, lanes, 0, ROWS), widen(vb, rv, j, lanes, 0, ROWS)))
    by_tile(filter_rows)
    g_rows(1, 0, BLK)
    dft(xh, 0, hs, 0)
    dft(xz, nblk, zs, nblk)
    z_rows(0, ROWS, BLK)
    dft(xg, 1, gs, 1)
    z_rows(1, 0, BLK)
    g_rows(2, 0, BLK)
    dft(xz, 2, zs, 2)
    learn(0)
    tell(1)
    z_rows(2, 0, BLK)
    dft(xg, 2, gs, 2)
    g_rows(last, 0, BLK)
    dft(xz, last, zs, last)
    dft(xg, last, gs, last)
    @pl.when(has_prev)
    def _():
        for copy in to_next:
            copy.wait_recv()

    def history(j, lanes):
        for raw, hist in ((rq, hq), (rk, hk), (rv, hv)):
            raw[j, 0:PAD, :] = hist[:, lanes].astype(F32)

    by_tile(history)
    z_rows(0, 0, ROWS, False)
    g_rows(0, 0, ROWS, False)
    dft(xz, 1, zs, 1)
    dft(xg, 0, gs, 0)

    def put_spectrum(ref, b, k, lanes, real, imag):
        for off, value in ((0, real), (BLK, imag)):
            high = value.astype(BF16)
            low = (value - high.astype(F32)).astype(BF16)
            ref[b, off + k : off + k + ROWS, lanes] = high
            ref[b, 2 * BLK + off + k : 2 * BLK + off + k + ROWS, lanes] = low
            ref[b, 4 * BLK + off + k : 4 * BLK + off + k + ROWS, lanes] = high

    def add(a, sign, b):
        return a + b if sign > 0 else a - b

    def frequencies():
        for k in range(0, BLK, ROWS):
            yield k, slice(k, k + ROWS), slice(BLK + k, BLK + k + ROWS), 1 if k < BLK // 2 else -1

    def z_stage(blocks, mode):
        def body(j, lanes):
            for k, re, im, sign in frequencies():
                hr, hi = hs[0, re, lanes], hs[0, im, lanes]
                lr = li = None
                if mode != "first":
                    lr, li = gl_f[re, lanes], gl_f[im, lanes]
                for b in blocks:
                    vr = add(zs[b + 1, re, lanes], -sign, zs[b, im, lanes])
                    vi = add(zs[b + 1, im, lanes], sign, zs[b, re, lanes])
                    gr, gi = gs[b, re, lanes], gs[b, im, lanes]
                    pr, pi = gr * vr + gi * vi, gi * vr - gr * vi
                    lr, li = (pr, pi) if lr is None else (lr + pr, li + pi)
                    put_spectrum(xs, b, k, lanes, hr * vr - hi * vi, hr * vi + hi * vr)
                if mode == "last":
                    put_spectrum(xgl, 0, k, lanes, lr, li)
                else:
                    gl_f[re, lanes] = lr
                    gl_f[im, lanes] = li

        by_tile(body)

    def g_stage(blocks):
        def body(j, lanes):
            for k, re, im, sign in frequencies():
                hr, hi = hs[0, re, lanes], hs[0, im, lanes]
                for b in blocks:
                    ur = add(gs[b, re, lanes], sign, gs[b + 1, im, lanes])
                    ui = add(gs[b, im, lanes], -sign, gs[b + 1, re, lanes])
                    put_spectrum(xu, b, k, lanes, hr * ur + hi * ui, hr * ui - hi * ur)

        by_tile(body)

    def inverse(x, b, use):
        for lane in range(0, width, 256):
            value = jnp.dot(inv[...], x[b, :, lane : lane + 256], preferred_element_type=F32)
            for part in range(0, 256, LANES):
                use(b, (lane + part) // LANES, value[:, part : part + LANES])

    def use_s(b, j, value):
        rows = slice(b * BLK, (b + 1) * BLK)
        gq[j, rows, :] = value * yb[rows, LANES * j : LANES * (j + 1)].astype(F32)

    def use_gz(b, j, value):
        rows = slice(b * BLK, (b + 1) * BLK)
        gk[j, rows, :] = value * vf[j, rows, :]
        gv[j, rows, :] = value * kf[j, rows, :]

    kinds = ((gq, rq, oq), (gk, rk, ok), (gv, rv, ov))

    def finish(which, r0, r1, fresh=False, write=True, count=True):
        grad, raw, out = kinds[which]

        def body(j, lanes):
            w = weights(which, lanes)
            sums = [None if fresh else taps[3 * which + i, j] for i in range(3)] if count else None
            for r in range(r0, r1, ROWS):
                own = grad[j, r : r + ROWS, :]
                if write:
                    one, two = grad[j, r + 1 : r + 1 + ROWS, :], grad[j, r + 2 : r + 2 + ROWS, :]
                    out[r : r + ROWS, lanes] = (w[0] * own + w[1] * one + w[2] * two).astype(BF16)
                if count:
                    for i in range(3):
                        product = own * raw[j, PAD + r - i : PAD + r - i + ROWS, :]
                        product = product[0:8] + product[8:16]
                        sums[i] = product if sums[i] is None else sums[i] + product
            if count:
                for i in range(3):
                    taps[3 * which + i, j] = sums[i]

        by_tile(body)

    z_stage((1,), "first")
    z_stage((2,), "more")
    inverse(xs, 1, use_s)
    z_stage((3,), "more")
    inverse(xs, 2, use_s)
    g_stage((0,))
    learn(1)
    tell(2)
    inverse(xs, 3, use_s)
    finish(0, BLK, 3 * BLK - ROWS, True)
    g_stage((1,))
    inverse(xu, 0, use_gz)
    finish(0, 3 * BLK - ROWS, length - ROWS)
    finish(0, length - ROWS, length, write=False)
    g_stage((2,))
    inverse(xu, 1, use_gz)
    finish(1, 0, BLK - ROWS, True)
    finish(2, 0, BLK - ROWS, True)
    inverse(xu, 2, use_gz)
    finish(1, BLK - ROWS, 2 * BLK - ROWS)
    finish(2, BLK - ROWS, 2 * BLK - ROWS)
    finish(1, 2 * BLK - ROWS, 3 * BLK - ROWS)
    finish(2, 2 * BLK - ROWS, 3 * BLK - ROWS)


    @pl.when(has_prev)
    def _():
        z_halo.wait_recv()

    @pl.when(has_next)
    def _():
        for copy in to_prev + g_halo:
            copy.wait_recv()

    share = BLK // total

    def next_rows(j, lanes):
        w = weights(0, lanes)
        rn[j, 0:PAD, :] = rq[j, length : length + PAD, :]
        rn[j, PAD : PAD + ROWS, :] = nq[:, lanes].astype(F32)
        put(xg, nblk, 0, lanes, ny[:, lanes].astype(F32) * feat(rn, j, w, 0, ROWS))

    def use_gl(b, j, value):
        cols = slice(LANES * j, LANES * (j + 1))
        for i in range(total):
            glt[i % 2, i // 2, :, cols] = value[share * i : share * (i + 1), :]
        half[j // 2, 2, 2 * (j % 2) + 1 : 2 * (j % 2) + 2, :] = value[0:1, :]

    xz[0, 2 * BLK :, :] = xz[0, 0:BLK, :]
    by_tile(next_rows)
    xg[nblk, 2 * BLK + ROWS :, :] = xg[nblk, ROWS:BLK, :]
    dft(xz, 0, zs, 0)
    dft(xg, nblk, gs, nblk)
    z_stage((0,), "last")
    g_stage((last,))
    inverse(xs, 0, use_s)
    inverse(xgl, 0, use_gl)
    inverse(xu, last, use_gz)
    row = lax.broadcasted_iota(jnp.int32, (8, LANES), 0)
    for j in range(tiles):
        second, third = pltpu.roll(gk[j, 0:8, :], 2, 0), pltpu.roll(gv[j, 0:8, :], 4, 0)
        mine3[j] = jnp.where(row < 2, gq[j, 0:8, :], jnp.where(row < 4, second, third))
    to_partner = remote(glt.at[1 - c], gl_in, 8, partner)
    to_partner.start()
    finish(0, 0, BLK)
    for which in (1, 2):
        finish(which, last * BLK - ROWS, length - ROWS)
        finish(which, length - ROWS, length, write=False)
    for j in range(tiles):
        h, jj = j // 2, j % 2
        for n in range(9):
            total_n = jnp.sum(taps[n, j], axis=0, keepdims=True)
            if n < 8:
                half[h, jj, n : n + 1, :] = total_n
            else:
                half[h, 2, 2 * jj : 2 * jj + 1, :] = total_n
    halves = remote(half.at[1 - c], half_in, 10, partner)
    halves.start()
    firsts = remote(mine3, nx, 9, prev)

    @pl.when(has_prev)
    def _():
        firsts.start()

    to_partner.wait_recv()
    racc[...] = glt[c] + gl_in[...]
    halves.wait_recv()
    group = min(4, chips)
    base = z // group * group
    place, mine = z - base, z // group
    groups = chips // group
    learn(2)
    far[mine] = half[c] + half_in[...]
    distant = []
    for d in sorted(range(1, groups), key=lambda d: -min(d, groups - d)):
        copy = remote(far.at[mine], far.at[mine], 20 + chips + d, at_chip(z + d * group))
        copy.start()
        distant.append(copy)
    scatter = []
    for d in sorted(range(1, chips), key=lambda d: (-min(d, chips - d), d)):
        chip = lax.rem(z + d, chips)
        copy = remote(racc.at[chip], rs_in.at[d], 16 + d, at_chip(chip))
        copy.start()
        scatter.append(copy)

    @pl.when(has_next)
    def _():
        firsts.wait_recv()

    for j in range(tiles):
        gq[j, length : length + 8, :] = nx[j]
        gk[j, length : length + 8, :] = pltpu.roll(nx[j], 6, 0)
        gv[j, length : length + 8, :] = pltpu.roll(nx[j], 4, 0)
    for which in range(3):
        finish(which, length - ROWS, length, count=False)

    for copy in distant:
        copy.wait_recv()
    summed = far[0]
    for n in range(1, groups):
        summed = summed + far[n]
    near[place] = summed
    close = []
    for d in range(1, group):
        copy = remote(near.at[place], near.at[place], 16 + chips + d, at_chip(base + lax.rem(place + d, group)))
        copy.start()
        close.append(copy)

    for copy in scatter:
        copy.wait_recv()
    mine_taps = racc[z]
    for d in range(1, chips):
        mine_taps = mine_taps + rs_in[d]
    ofilt[...] = mine_taps

    for copy in close:
        copy.wait_recv()
    whole = near[0]
    for n in range(1, group):
        whole = whole + near[n]
    fin[c] = whole
    final = remote(fin.at[c], fin.at[c], 11, partner)
    final.start()
    final.wait_recv()
    for h in range(2):
        for j in range(2):
            cols = slice(256 * h + 128 * j, 256 * h + 128 * (j + 1))
            for i in range(8):
                otaps[i // 3, i % 3 : i % 3 + 1, cols] = fin[h, j, i : i + 1, :]
            otaps[2, 2:3, cols] = fin[h, 2, 2 * j : 2 * j + 1, :]
            ogain[0:1, cols] = fin[h, 2, 2 * j + 1 : 2 * j + 2, :]

    @pl.when(has_next)
    def _():
        for copy in to_next:
            copy.wait_send()
        z_halo.wait_send()

    @pl.when(has_prev)
    def _():
        for copy in to_prev + g_halo + [firsts]:
            copy.wait_send()

    for copy in [to_partner, halves, final] + close + distant + scatter:
        copy.wait_send()


def put_out(*refs):
    sem = refs[-1]
    copies = [pltpu.make_async_copy(refs[n], refs[n + 6], sem.at[n]) for n in range(6)]
    for copy in copies:
        copy.start()
    for copy in copies:
        copy.wait()


def body(fwd, inv, chips, input_q, input_k, input_v, grad_out, short_filters, long_filter, skip_gain):
    length, width = input_q.shape
    nblk = length // BLK
    hbm = pl.BlockSpec(memory_space=pltpu.HBM)
    vmem = pl.BlockSpec(memory_space=pltpu.VMEM)
    tiles = width // LANES
    share = BLK // (2 * chips)
    scratch = [
        *(pltpu.VMEM((length, width), BF16) for _ in range(4)),
        *(pltpu.VMEM((PAD, width), BF16) for _ in range(3)),
        *(pltpu.VMEM((ROWS, width), BF16) for _ in range(2)),
        pltpu.VMEM(short_filters.shape, F32),
        pltpu.VMEM(long_filter.shape, F32),
        pltpu.VMEM((1, width), F32),
        pltpu.VMEM(fwd.shape, BF16),
        pltpu.VMEM(inv.shape, BF16),
        *(pltpu.VMEM((tiles, PAD + length, LANES), F32) for _ in range(3)),
        pltpu.VMEM((tiles, PAD + ROWS, LANES), F32),
        *(pltpu.VMEM((tiles, length, LANES), F32) for _ in range(2)),
        *(pltpu.VMEM((tiles, length + 8, LANES), F32) for _ in range(3)),
        pltpu.VMEM((nblk + 1, 3 * BLK, width), BF16),
        pltpu.VMEM((nblk + 1, 3 * BLK, width), BF16),
        pltpu.VMEM((1, 3 * BLK, width), BF16),
        pltpu.VMEM((nblk + 1, 2 * BLK, width), F32),
        pltpu.VMEM((nblk + 1, 2 * BLK, width), F32),
        pltpu.VMEM((1, 2 * BLK, width), F32),
        pltpu.VMEM((nblk, 6 * BLK, width), BF16),
        pltpu.VMEM((nblk, 6 * BLK, width), BF16),
        pltpu.VMEM((2 * BLK, width), F32),
        pltpu.VMEM((1, 6 * BLK, width), BF16),
        pltpu.VMEM((tiles, 8, LANES), F32),
        pltpu.VMEM((tiles, 8, LANES), F32),
        pltpu.VMEM((2, chips, share, width), F32),
        pltpu.VMEM((chips, share, width), F32),
        pltpu.VMEM((chips, share, width), F32),
        pltpu.VMEM((chips, share, width), F32),
        pltpu.VMEM((9, tiles, 8, LANES), F32),
        pltpu.VMEM((2, 3, 8, LANES), F32),
        pltpu.VMEM((3, 8, LANES), F32),
        pltpu.VMEM((4, 3, 8, LANES), F32),
        pltpu.VMEM((4, 3, 8, LANES), F32),
        pltpu.VMEM((2, 3, 8, LANES), F32),
        pltpu.SemaphoreType.DMA((4 * nblk + 5,)),
        pltpu.SemaphoreType.DMA((32 + chips,)),
        pltpu.SemaphoreType.DMA((32 + chips,)),
        pltpu.SemaphoreType.REGULAR((3,)),
    ]
    operands = (input_q, input_k, input_v, grad_out, short_filters, long_filter, skip_gain[None], fwd, inv)
    outs = pl.pallas_call(
        functools.partial(kernel, chips),
        out_shape=(
            *(pltpu.VMEM((length, width), BF16) for _ in range(3)),
            pltpu.VMEM((BLK // (2 * chips), width), F32),
            pltpu.VMEM(short_filters.shape, F32),
            pltpu.VMEM((1, width), F32),
        ),
        in_specs=[hbm] * 9,
        out_specs=(vmem,) * 6,
        scratch_shapes=scratch,
        compiler_params=pltpu.CompilerParams(
            collective_id=0, has_side_effects=True, vmem_limit_bytes=48 * 1024 * 1024
        ),
        name="hyena_backward",
    )(*(pltpu.with_memory_space_constraint(a, pltpu.HBM) for a in operands))
    done = pl.pallas_call(
        put_out,
        out_shape=tuple(jax.ShapeDtypeStruct(o.shape, o.dtype) for o in outs),
        in_specs=[vmem] * 6,
        out_specs=(hbm,) * 6,
        scratch_shapes=[pltpu.SemaphoreType.DMA((6,))],
        compiler_params=pltpu.CompilerParams(vmem_limit_bytes=1 << 20),
        name="put_out",
    )(*outs)
    return (*done[:5], done[5][0])


def solution(mesh):
    chips = mesh.shape["seq"] // 2
    fwd, inv = tables()

    def run(*arrays):
        return body(jnp.asarray(fwd), jnp.asarray(inv), chips, *arrays)

    return jax.shard_map(
        run,
        mesh=mesh,
        in_specs=(
            P("seq", "ch"),
            P("seq", "ch"),
            P("seq", "ch"),
            P("seq", "ch"),
            P(None, None, "ch"),
            P(None, "ch"),
            P("ch"),
        ),
        out_specs=(
            P("seq", "ch"),
            P("seq", "ch"),
            P("seq", "ch"),
            P("seq", "ch"),
            P(None, None, "ch"),
            P("ch"),
        ),
        check_vma=False,
    )
```
